32 devices in a mesh: expert: 8 (over y, x, core), tensor: 4 (over z).
Axes of the slice: x: 2, y: 2, z: 4, core: 2. Of those that a mesh axis runs over, the one named last changes fastest.
Arguments:
- hidden_in: bfloat16 [2048, 2048], P('expert'), may hold values from -6 to 6
- segment_ids: int32 [8, 256], P('expert'), may hold values from 0 to 1, never falling along the last dimension, each value on 1 to 192 neighbouring positions
- expert_ids: int32 [2048, 6], P('expert'), may hold values from 0 to 15, all different within a row; in each aligned block of 256 rows (0 to 255, 256 to 511, ...) at most 192 rows name the same one
- query_weight: bfloat16 [2048, 3072], P('expert', 'tensor')
- latent_weight: bfloat16 [2048, 576], P('expert')
- expand_weight: bfloat16 [512, 4096], P('expert', 'tensor'), may hold values from -0.25 to 0.25
- output_weight: bfloat16 [2048, 2048], P('tensor', 'expert'), may hold values from -1 to 1
- prenorm: bfloat16 [2048], P('expert'), may hold values from 0.25 to 1.75
- latentnorm: bfloat16 [512], P('expert'), may hold values from 0.25 to 1.75
- postnorm: bfloat16 [2048], P('expert'), may hold values from 0.25 to 1.75
- router_weight: bfloat16 [2048, 16], P('expert'), may hold values from -0.125 to 0.125
- shared_gate: bfloat16 [2048, 2816], P('expert', 'tensor'), may hold values from -0.125 to 0.125
- shared_up: bfloat16 [2048, 2816], P('expert', 'tensor'), may hold values from -0.125 to 0.125
- shared_down: bfloat16 [2816, 2048], P('tensor', 'expert'), may hold values from -0.109375 to 0.109375
- expert_gate: bfloat16 [16, 2048, 1408], P('expert', None, 'tensor'), may hold values from -0.125 to 0.125
- expert_up: bfloat16 [16, 2048, 1408], P('expert', None, 'tensor'), may hold values from -0.125 to 0.125
- expert_down: bfloat16 [16, 1408, 2048], P('expert', 'tensor'), may hold values from -0.15625 to 0.15625
- cotangent: bfloat16 [2048, 2048], P('expert'), may hold values from -6 to 6
Outputs:
- block_output: bfloat16 [2048, 2048], P('expert')
- input_gradient: bfloat16 [2048, 2048], P('expert')
- query_gradient: float32 [2048, 3072], P('expert', 'tensor')
- latent_gradient: float32 [2048, 576], P('expert')
- expand_gradient: float32 [512, 4096], P('expert', 'tensor')
- output_gradient: float32 [2048, 2048], P('tensor', 'expert')
- prenorm_gradient: float32 [2048], P('expert')
- latentnorm_gradient: float32 [512], P('expert')
- postnorm_gradient: float32 [2048], P('expert')
- router_gradient: float32 [2048, 16], P('expert')
- shared_gate_gradient: float32 [2048, 2816], P('expert', 'tensor')
- shared_up_gradient: float32 [2048, 2816], P('expert', 'tensor')
- shared_down_gradient: float32 [2816, 2048], P('tensor', 'expert')
- expert_gate_gradient: float32 [16, 2048, 1408], P('expert', None, 'tensor')
- expert_up_gradient: float32 [16, 2048, 1408], P('expert', None, 'tensor')
- expert_down_gradient: float32 [16, 1408, 2048], P('expert', 'tensor')
The draws below stay inside these ranges and needn't reach their ends.
Inputs may be any that keep to these rules, and one draw needn't show every extreme that they name: `segment_ids`: each sequence holds two documents, numbered 0 then 1: one of 64 to 192 positions and one of the rest, in either order. `expert_ids`: within the 256 rows of one sequence at most 192 pairs name any one expert, a bound that some block reaches.
All inputs are finite; a program needn't handle non-finite values.
Results may differ from the reference program's by a relative error of at most 0.025.
Values may be sent and summed in bfloat16 or wider, within the bound.
A program may use at most 320 MiB of HBM per device.

```python
import math
import jax
import jax.numpy as jnp
import numpy as np
from jax import lax

D = 2048
HEADS = 16
HEAD_DIM = 128
ROPE_DIM = 64
KV_RANK = 512
MOE_FF = 1408
SHARED_FF = 2816
TOP = 6
TOK_DEV = 256
SEQS = 8
TOKENS = 2048
EXPERTS = 16
CAP = 192
N_TENSOR = 4


def projection_pair(key):
    latent = jax.random.truncated_normal(jax.random.fold_in(key, 11), -4.0, 4.0, (D, KV_RANK + ROPE_DIM), jnp.float32) / math.sqrt(D)
    queries = jax.random.truncated_normal(jax.random.fold_in(key, 12), -4.0, 4.0, (D, HEADS, HEAD_DIM + ROPE_DIM), jnp.float32) / math.sqrt(D)
    return (queries.reshape(D, HEADS * (HEAD_DIM + ROPE_DIM)), latent)


def draw_query_weight(key, part):
    return projection_pair(key)[0].astype(jnp.bfloat16)


def draw_latent_weight(key, part):
    return projection_pair(key)[1].astype(jnp.bfloat16)


def block_levels(rng, extent, cuts, low, high):
    level, own = 1.0, jax.random.fold_in(rng, 6)
    for dim, shards_of in cuts:
        draws = jnp.exp(jax.random.uniform(jax.random.fold_in(own, dim), (shards_of,), jnp.float32, low / len(cuts), high / len(cuts)))
        level = level * jnp.repeat(draws, extent[dim] // shards_of).reshape([-1 if axis == dim else 1 for axis in range(len(extent))])
    return level


def split_up(number_of, total, limit, skew):
    loads = [(1 << 20) // math.isqrt(standing ** skew) + 1 for standing in range(2, number_of + 1)]
    surplus, holding = total - limit - (number_of - 1), [1] * (number_of - 1)
    while surplus > 0:
        movable = [i for i in range(number_of - 1) if holding[i] < limit]
        mass, remaining = sum([loads[i] for i in movable]), surplus
        for i in movable:
            more = min(limit - holding[i], max(1, remaining * loads[i] // mass), surplus)
            holding[i] = holding[i] + more
            surplus = surplus - more
    return np.array([limit] + holding)


def ragged(rng, amount, total, most, slope):
    if amount == 2:
        one = jax.random.randint(rng, (), max(1, total - most), min(most, total - 1) + 1)
        return jnp.stack([one, total - one])
    sizes = jnp.asarray(split_up(amount, total, most, slope), jnp.int32)
    couples = (amount - 1) // 2
    source_of, receiver = sizes[1:1 + 2 * couples:2], sizes[2:2 + 2 * couples:2]
    margin = jnp.minimum(source_of - 1, most - receiver)
    shifted = jax.random.randint(jax.random.fold_in(rng, 1), (couples,), 0, 1 << 20) % (margin + 1)
    sizes = sizes.at[1:1 + 2 * couples:2].set(source_of - shifted).at[2:2 + 2 * couples:2].set(receiver + shifted)
    return sizes[jax.random.permutation(jax.random.fold_in(rng, 2), amount)]


def routed_block(own_key, own, number, rows, amount, top, reach, slope):
    order = jax.random.permutation(own_key, amount)
    heavy_load, usual = shares(amount, rows * top, reach, slope, True), shares(amount, rows * top, reach, slope, False)
    places = jnp.arange(amount)

    def named(tallies, rotation):
        used = int((tallies > 0).sum())
        fixed = max(1, used // 4)
        moved = fixed + (places - fixed + rotation * (used - fixed)) % max(1, amount - fixed)
        return jnp.zeros((amount,), jnp.int32).at[order[jnp.where(places < fixed, places, moved)]].set(jnp.asarray(tallies, jnp.int32))

    tallies = jnp.where(number % 4 == 0, named(heavy_load, number // 4), named(usual, number - number // 4 - 1))
    mixed = jax.random.permutation(jax.random.fold_in(own, 3), amount)
    donor, sink = mixed[0:amount // 2 * 2:2], mixed[1:amount // 2 * 2:2]
    slack = jnp.minimum(tallies[donor] - 1, reach - tallies[sink]) // 2
    slack = jnp.where((donor == order[0]) | (sink == order[0]) | (tallies[sink] == 0), 0, jnp.maximum(slack, 0))
    moved = jax.random.randint(jax.random.fold_in(own, 4), (amount // 2,), 0, 1 << 20) % (slack + 1)
    tallies = tallies.at[donor].add(-moved).at[sink].add(moved)
    items = jnp.searchsorted(jnp.cumsum(tallies), jnp.arange(rows * top), side="right").astype(jnp.int32)
    listing = items.reshape(top, rows).T
    listing = listing[jax.random.permutation(jax.random.fold_in(own, 1), rows)]
    rotation = jax.random.randint(jax.random.fold_in(own, 2), (rows, 1), 0, top)
    return jnp.take_along_axis(listing, (jnp.arange(top)[None, :] + rotation) % top, axis=1)


def shares(number_of, total, bound, lean, full):
    weights = [(1 << 20) // math.isqrt(rank ** lean) + 1 for rank in range(1, number_of + 1)]
    largest = bound if full else min(bound, max(-(-total // number_of), total * weights[0] // sum(weights)))
    least = 1 if total - largest >= number_of - 1 else 0
    holding, spare = [largest] + [least] * (number_of - 1), total - largest - least * (number_of - 1)
    while spare > 0:
        free = [i for i in range(1, number_of) if holding[i] < largest] or [i for i in range(1, number_of) if holding[i] < bound]
        mass, budget = sum([weights[i] for i in free]), spare
        for i in free:
            more = min(bound - holding[i], max(1, budget * weights[i] // mass), spare)
            holding[i] = holding[i] + more
            spare = spare - more
    return np.array(holding)


def scatter_about(key, shape, scale, bound, cuts=(), held_as=jnp.bfloat16):
    factor_of = block_levels(key, shape, cuts, -0.22, 0.18) if cuts else 1.0
    result = jax.random.normal(key, shape, jnp.float32) * scale * factor_of
    return jnp.minimum(jnp.maximum(result, -bound), bound).astype(held_as)


def setup_inputs(seed: int = 0) -> dict:
    splits = jax.random.split(jax.random.key(seed), 19)
    hidden_in = scatter_about(splits[0], (TOKENS, D), 1.0, 6.0, ((0, 8),))
    segment_ids = jax.vmap(lambda own: jnp.searchsorted(jnp.cumsum(ragged(own, 2, TOK_DEV, TOK_DEV * 3 // 4, 2)), jnp.arange(TOK_DEV), side="right"))(jax.random.split(splits[1], SEQS)).reshape((SEQS, TOK_DEV)).astype(jnp.int32)
    expert_ids_keys = jax.random.split(jax.random.fold_in(splits[2], 1), TOKENS // TOK_DEV)
    expert_ids_turns = jax.random.permutation(jax.random.fold_in(splits[2], 3), TOKENS // TOK_DEV)
    expert_ids = jax.vmap(lambda own, number: routed_block(jax.random.fold_in(splits[2], 2), own, number, TOK_DEV, EXPERTS, TOP, CAP, 2))(expert_ids_keys, expert_ids_turns).reshape((TOKENS, TOP))
    query_weight = draw_query_weight(jax.random.fold_in(splits[18], 71), 0)
    latent_weight = draw_latent_weight(jax.random.fold_in(splits[18], 71), 0)
    expand_weight = scatter_about(splits[5], (KV_RANK, HEADS * 2 * HEAD_DIM), KV_RANK ** -0.5, 0.25, ((0, 8), (1, 4)))
    output_weight = scatter_about(splits[6], (HEADS * HEAD_DIM, D), (max(1, HEADS * HEAD_DIM // 64)) ** -0.5, 1.0, ((0, 4), (1, 8)))
    prenorm = jnp.clip(1.0 + 0.15 * jax.random.normal(splits[7], (D,), jnp.float32), 0.25, 1.75).astype(jnp.bfloat16)
    latentnorm = jnp.clip(1.0 + 0.15 * jax.random.normal(splits[8], (KV_RANK,), jnp.float32), 0.25, 1.75).astype(jnp.bfloat16)
    postnorm = jnp.clip(1.0 + 0.15 * jax.random.normal(splits[9], (D,), jnp.float32), 0.25, 1.75).astype(jnp.bfloat16)
    router_weight = scatter_about(splits[10], (D, EXPERTS), D ** -0.5, 0.125, ((0, 8),))
    shared_gate = scatter_about(splits[11], (D, SHARED_FF), D ** -0.5, 0.125, ((0, 8), (1, 4)))
    shared_up = scatter_about(splits[12], (D, SHARED_FF), D ** -0.5, 0.125, ((0, 8), (1, 4)))
    shared_down = scatter_about(splits[13], (SHARED_FF, D), SHARED_FF ** -0.5, 0.109375, ((0, 4), (1, 8)))
    expert_gate = scatter_about(splits[14], (EXPERTS, D, MOE_FF), D ** -0.5, 0.125, ((0, 8), (2, 4)))
    expert_up = scatter_about(splits[15], (EXPERTS, D, MOE_FF), D ** -0.5, 0.125, ((0, 8), (2, 4)))
    expert_down = scatter_about(splits[16], (EXPERTS, MOE_FF, D), MOE_FF ** -0.5, 0.15625, ((0, 8), (1, 4)))
    cotangent = scatter_about(splits[17], (TOKENS, D), 1.0, 6.0, ((0, 8),))
    return dict(hidden_in=hidden_in, segment_ids=segment_ids, expert_ids=expert_ids, query_weight=query_weight, latent_weight=latent_weight, expand_weight=expand_weight, output_weight=output_weight, prenorm=prenorm, latentnorm=latentnorm, postnorm=postnorm, router_weight=router_weight, shared_gate=shared_gate, shared_up=shared_up, shared_down=shared_down, expert_gate=expert_gate, expert_up=expert_up, expert_down=expert_down, cotangent=cotangent)


@jax.custom_vjp
def low(v):
    return lax.optimization_barrier(v.astype(jnp.bfloat16)).astype(jnp.float32)

@jax.custom_vjp
def low_back(v):
    return v

def low_keep(v):
    return (low(v), None)

def low_pass(kept, grad):
    return (grad,)

def back_keep(v):
    return (v, None)

def back_low(kept, grad):
    return (low(grad),)
low.defvjp(low_keep, low_pass)
low_back.defvjp(back_keep, back_low)
EPSILON = 1e-06
ROUTE_SCALE = 2.446
ROPE_BASE = 50000.0
MASKED = -1e+30
HIGHEST = lax.Precision.HIGHEST

def product(left, right):
    return jnp.dot(left, right, precision=HIGHEST, preferred_element_type=jnp.float32)

def rms_scale(values, gain):
    square_mean = lax.optimization_barrier(jnp.mean(values * values, axis=-1, keepdims=True))
    return values * lax.rsqrt(square_mean + EPSILON) * gain

def rotary_tables(length):
    position = jnp.arange(length).astype(jnp.float32)
    exponent = jnp.arange(ROPE_DIM // 2).astype(jnp.float32) * (2.0 / ROPE_DIM)
    angles = position[:, None] * jnp.exp(-math.log(ROPE_BASE) * exponent)[None, :]
    return (jnp.cos(angles), jnp.sin(angles))

def rotate(values, cosine, sine):
    half = values.shape[-1] // 2
    first = values[..., :half]
    second = values[..., half:]
    return jnp.concatenate([first * cosine - second * sine, second * cosine + first * sine], axis=-1)

def sigmoid(values):
    return 1.0 / (1.0 + jnp.exp(-values))

def slot_numbers(choices):
    flat_choice = choices.reshape(-1)
    onehot = (flat_choice[:, None] == jnp.arange(EXPERTS).astype(jnp.int32)[None, :]).astype(jnp.int32)
    earlier = jnp.cumsum(onehot, axis=0) - onehot
    return lax.optimization_barrier(jnp.sum(earlier * onehot, axis=1)).astype(jnp.int32).reshape(choices.shape)

def block(params, hidden, segments, choices):
    query_weight, latent_weight, expand_weight, output_weight, pre_gain, latent_gain, post_gain, router_weight, common_gate, common_up, common_down, routed_gate_weight, routed_up_weight, routed_down_weight = params
    length = hidden.shape[0]
    cosine, sine = rotary_tables(length)
    normed = low(rms_scale(hidden, pre_gain))
    query_raw = low_back(product(normed, query_weight)).reshape(length, HEADS, HEAD_DIM + ROPE_DIM)
    query_nope = low(query_raw[..., :HEAD_DIM])
    query_rope = low(rotate(query_raw[..., HEAD_DIM:], cosine[:, None, :], sine[:, None, :]))
    latent_all = low_back(product(normed, latent_weight))
    compressed = low(rms_scale(latent_all[:, :KV_RANK], latent_gain))
    key_rope = low(rotate(latent_all[:, KV_RANK:], cosine, sine))
    expanded = low(low_back(product(compressed, expand_weight))).reshape(length, HEADS, 2 * HEAD_DIM)
    key_nope = expanded[..., :HEAD_DIM]
    values = expanded[..., HEAD_DIM:]
    scale = 1.0 / math.sqrt(HEAD_DIM + ROPE_DIM)
    scores = jnp.einsum('qhd,khd->hqk', query_nope, key_nope, precision=HIGHEST)
    scores = scores + jnp.einsum('qhr,kr->hqk', query_rope, key_rope, precision=HIGHEST)
    position = jnp.arange(length)
    allowed = (position[None, :] <= position[:, None]) & (segments[:, None] == segments[None, :])
    scores = low_back(jnp.where(allowed[None], scores * scale, MASKED))
    maxima = lax.optimization_barrier(jnp.max(scores, axis=2, keepdims=True))
    weights = jnp.exp(scores - maxima)
    probabilities = weights / lax.optimization_barrier(jnp.sum(weights, axis=2, keepdims=True))
    attended = low(low_back(jnp.einsum('hqk,khd->qhd', low(probabilities), values, precision=HIGHEST)))
    attention = low_back(product(attended.reshape(length, HEADS * HEAD_DIM), output_weight))
    middle = hidden + attention
    normed_mid = low(rms_scale(middle, post_gain))
    affinity = sigmoid(low_back(product(normed_mid, router_weight)))
    selected = jnp.take_along_axis(affinity, choices, axis=1)
    mixing = ROUTE_SCALE * selected / lax.optimization_barrier(jnp.sum(selected, axis=1, keepdims=True))
    gate_pre = low_back(product(normed_mid, common_gate))
    up_pre = low_back(product(normed_mid, common_up))
    shared_hidden = low(gate_pre * sigmoid(gate_pre) * up_pre)
    shared_out = low_back(product(shared_hidden, common_down))
    slots = slot_numbers(choices)
    flat_rows = (choices * CAP + slots).reshape(-1)
    buffer = jnp.zeros((EXPERTS * CAP, D), jnp.float32).at[flat_rows].set(jnp.repeat(normed_mid, TOP, axis=0))
    grouped = low_back(jnp.broadcast_to(buffer.reshape(EXPERTS, CAP, 1, D), (EXPERTS, CAP, N_TENSOR, D)))
    share = MOE_FF // N_TENSOR
    gate_routed = low_back(jnp.einsum('ecgd,edgf->ecgf', grouped, routed_gate_weight.reshape(EXPERTS, D, N_TENSOR, share), precision=HIGHEST))
    up_routed = low_back(jnp.einsum('ecgd,edgf->ecgf', grouped, routed_up_weight.reshape(EXPERTS, D, N_TENSOR, share), precision=HIGHEST))
    routed_hidden = low(gate_routed * sigmoid(gate_routed) * up_routed)
    partial_value = low(jnp.einsum('ecgf,egfd->ecgd', routed_hidden, routed_down_weight.reshape(EXPERTS, N_TENSOR, share, D), precision=HIGHEST))
    combined = lax.optimization_barrier(jnp.sum(partial_value, axis=2)).reshape(EXPERTS * CAP, D)
    returned = low_back(combined[flat_rows].reshape(length, TOP, D))
    routed_out = lax.optimization_barrier(jnp.sum(returned * mixing[:, :, None], axis=1))
    return middle + shared_out + routed_out

def reference(hidden_in, segment_ids, expert_ids, query_weight, latent_weight, expand_weight, output_weight, prenorm, latentnorm, postnorm, router_weight, shared_gate, shared_up, shared_down, expert_gate, expert_up, expert_down, cotangent):
    params = tuple((weight.astype(jnp.float32) for weight in (query_weight, latent_weight, expand_weight, output_weight, prenorm, latentnorm, postnorm, router_weight, shared_gate, shared_up, shared_down, expert_gate, expert_up, expert_down)))
    hidden = hidden_in.astype(jnp.float32).reshape(SEQS, TOK_DEV, D)
    choices = expert_ids.reshape(SEQS, TOK_DEV, TOP)
    checked = jax.checkpoint(block)

    def forward(weights, inputs):

        def one_sequence(carry, sequence):
            return (carry, checked(weights, sequence[0], sequence[1], sequence[2]))
        unused, outputs = lax.scan(one_sequence, jnp.zeros((), jnp.float32), (inputs, segment_ids, choices))
        return outputs
    outputs, pullback = jax.vjp(forward, params, hidden)
    weight_grads, hidden_grad = pullback(cotangent.astype(jnp.float32).reshape(SEQS, TOK_DEV, D))
    query_out, latent_out, expand_out, output_out, pre_out, latent_norm_out, post_out, router_out, gate_out, up_out, down_out, routed_gate_out, routed_up_out, routed_down_out = weight_grads
    return (outputs.reshape(TOKENS, D).astype(jnp.bfloat16), hidden_grad.reshape(TOKENS, D).astype(jnp.bfloat16), query_out, latent_out, expand_out, output_out, pre_out, latent_norm_out, post_out, router_out, gate_out, up_out, down_out, routed_gate_out, routed_up_out, routed_down_out)
```

```python
import math

import jax
import jax.numpy as jnp
from jax import lax
from jax.experimental import pallas as pl
from jax.experimental.pallas import tpu as pltpu
from jax.sharding import PartitionSpec as P

D = 2048
HEAD_DIM = 128
ROPE_DIM = 64
KV_RANK = 512
TOP = 6


EPSILON = 1e-06
ROUTE_SCALE = 2.446
ROPE_BASE = 50000.0
MASKED = -1e30


def matmul(left, right):
    return jnp.dot(left, right, preferred_element_type=jnp.float32)


def matmul_nt(left, right):
    return lax.dot_general(
        left, right, (((1,), (1,)), ((), ())), preferred_element_type=jnp.float32
    )


def matmul_tn(left, right):
    return lax.dot_general(
        left, right, (((0,), (0,)), ((), ())), preferred_element_type=jnp.float32
    )


def rotary_tables(length):
    position = jnp.arange(length).astype(jnp.float32)
    exponent = jnp.arange(ROPE_DIM // 2).astype(jnp.float32) * (2.0 / ROPE_DIM)
    angles = position[:, None] * jnp.exp(-math.log(ROPE_BASE) * exponent)[None, :]
    return (jnp.cos(angles), jnp.sin(angles))


def rotate(values, cosine, sine):
    half = values.shape[-1] // 2
    first = values[..., :half]
    second = values[..., half:]
    return jnp.concatenate(
        [first * cosine - second * sine, second * cosine + first * sine], axis=-1
    )


def sigmoid(values):
    return 1.0 / (1.0 + jnp.exp(-values))


def norm_backward(grad_normed, values, inverse, gain):
    gain_grad = jnp.sum(grad_normed * values * inverse, axis=0)
    scaled = grad_normed * gain
    inner = jnp.mean(scaled * values, axis=1, keepdims=True)
    return (inverse * scaled - values * inverse * inverse * inverse * inner, gain_grad)


MESH = pl.DeviceIdType.MESH
ANY = pl.BlockSpec(memory_space=pl.ANY)
VMEM = pl.BlockSpec(memory_space=pltpu.VMEM)


def xor_bit(value, bit):
    return value + bit - 2 * bit * lax.rem(value // bit, 2)


def add_rows(dst, first, second, rows):
    step = math.gcd(rows, 16)

    def body(i, carry):
        at = pl.ds(pl.multiple_of(i * step, step), step)
        total = first[at].astype(jnp.float32) + second[at].astype(jnp.float32)
        dst[at] = total.astype(dst.dtype)
        return carry

    lax.fori_loop(0, rows // step, body, 0)


class Fabric:
    def __init__(self, send, recv, local):
        self.send, self.recv, self.local = send, recv, local
        self.used = self.local_used = 0
        self.e = lax.axis_index("expert")
        self.z = lax.axis_index("tensor")
        self.partner = (xor_bit(self.e, 1), self.z)
        self.xn = (xor_bit(self.e, 2), self.z)
        self.yn = (xor_bit(self.e, 4), self.z)
        self.line = (self.e, xor_bit(self.z, 1))
        self.middle = (self.e, 3 - self.z)
        self.inner = jnp.logical_or(self.z == 1, self.z == 2)

    def copy(self, src, dst, device):
        k = self.used
        self.used += 1
        return pltpu.make_async_remote_copy(
            src_ref=src,
            dst_ref=dst,
            send_sem=self.send.at[k],
            recv_sem=self.recv.at[k],
            device_id=device,
            device_id_type=MESH,
        )

    def here(self, src, dst):
        k = self.local_used
        self.local_used += 1
        return pltpu.make_async_copy(src, dst, self.local.at[k])

    def slot(self, bits):
        e = self.e
        for bit in (1, 2, 4):
            if bits & bit:
                e = xor_bit(e, bit)
        return e


class Gather:
    sends, locals = 9, 2

    def __init__(self, array, axis=0, at=0.0, early=False):
        self.array, self.axis, self.at, self.early = array, axis, at, early
        r, c = array.shape
        shape = (r, 8 * c) if axis else (8, r, c)
        self.arrays, self.outs = [array], [jax.ShapeDtypeStruct(shape, array.dtype)]
        self.in_spec = self.out_spec = ANY
        self.scratch = [pltpu.VMEM(array.shape, array.dtype)]
        self.span = self.load = 3 * 2 * array.size * array.dtype.itemsize / 160e3

    def finish(self):
        return self.at + self.wait + self.load + 5.0

    def plain(self):
        return [lax.all_gather(self.array, "expert", axis=self.axis, tiled=bool(self.axis))]

    def steps(self, fab, src, dst, held):
        r, c = self.array.shape
        h = (r // 2 + 15) // 16 * 16 if r > 16 else r // 2
        parts = {0: pl.ds(0, h), 1: pl.ds(h, r - h), None: pl.ds(0, r)}

        def view(bits, part=None):
            slot = fab.slot(bits)
            if self.axis:
                return dst.at[parts[part], pl.ds(pl.multiple_of(slot * c, c), c)]
            return dst.at[slot, parts[part]]

        def forward(bits, device, part=None):
            return fab.copy(view(bits, part), view(bits, part), device)

        load, store = fab.here(src, held), fab.here(held, view(0))
        to_x, to_y, to_p = (fab.copy(src, view(0), d) for d in (fab.xn, fab.yn, fab.partner))
        lo, hi = forward(2, fab.yn, 0), forward(4, fab.xn, 1)
        px, py = forward(2, fab.partner), forward(4, fab.partner)
        plo, phi = forward(6, fab.partner, 0), forward(6, fab.partner, 1)

        def begin():
            for each in (to_x, to_y, to_p, load):
                each.start()

        def keep():
            load.wait()
            store.start()

        def from_x():
            to_x.wait_recv()
            lo.start()
            px.start()

        def from_y():
            to_y.wait_recv()
            hi.start()
            py.start()

        def corner_lo():
            lo.wait_recv()
            plo.start()

        def corner_hi():
            hi.wait_recv()
            phi.start()

        def arrive():
            store.wait()
            for each in (to_p, px, py, plo, phi):
                each.wait_recv()

        def end():
            for each in (to_x, to_y, to_p, lo, hi, px, py, plo, phi):
                each.wait_send()

        t, s, w = self.at, self.span, self.wait
        return [
            (self.start, begin),
            (self.start + 2, keep),
            (t + w + 2 + s * 2 / 3, from_x),
            (t + w + 2 + s * 2 / 3, from_y),
            (t + w + 3 + s, corner_lo),
            (t + w + 3 + s, corner_hi),
            (self.finish() if self.early else 1e8, arrive),
            (1e9, end),
        ]


class Swap:
    sends, locals = 7, 2

    def __init__(self, array, at=0.0):
        self.array, self.at = array, at
        self.arrays, self.outs = [array], [jax.ShapeDtypeStruct(array.shape, array.dtype)]
        self.in_spec = self.out_spec = ANY
        self.scratch = [pltpu.VMEM(array.shape[1:], array.dtype)]
        self.load = array.size * array.dtype.itemsize / 80e3

    def plain(self):
        return [lax.all_to_all(self.array, "expert", split_axis=0, concat_axis=0, tiled=True)]

    def steps(self, fab, src, dst, held):
        e = fab.e
        load, store = fab.here(src.at[e], held), fab.here(held, dst.at[e])
        copies = []
        for bits in (6, 7, 2, 3, 4, 5, 1):
            other = fab.slot(bits)
            copies.append(fab.copy(src.at[other], dst.at[e], (other, fab.z)))

        def begin():
            for each in copies:
                each.start()
            load.start()

        def keep():
            load.wait()
            store.start()

        def end():
            store.wait()
            for each in copies:
                each.wait()

        return [(self.start, begin), (self.start + 2, keep), (1e9, end)]


class Scatter:
    def __init__(self, array, axis=0, pieces=1, at=0.0, out_dtype=None, source=None):
        self.array, self.axis, self.pieces, self.at, self.source = array, axis, pieces, at, source
        if axis:
            r, c = array.shape[0], array.shape[1] // 8
        else:
            r, c = array.shape[1:]
        self.r, self.c = r, c
        self.arrays, self.outs = [array], [jax.ShapeDtypeStruct((r, c), out_dtype or array.dtype)]
        if source:
            self.arrays = []
        self.in_spec, self.out_spec = ANY, VMEM
        d = array.dtype
        self.scratch = [
            pltpu.VMEM((4, r, c), d),
            pltpu.VMEM((4, r, c), d),
            pltpu.VMEM((2, r, c), d),
            pltpu.VMEM((r, c), d),
            pltpu.VMEM((r, c), d),
        ]
        self.sends, self.locals = 10 * pieces, 4 * pieces
        self.load = 3 * 2 * r * c * d.itemsize / 160e3
        self.span = self.load / pieces

    def plain(self):
        if self.axis:
            out = lax.psum_scatter(self.array, "expert", scatter_dimension=1, tiled=True)
        else:
            out = lax.psum_scatter(self.array, "expert", scatter_dimension=0, tiled=False)
        return [out.astype(self.outs[0].dtype)]

    def steps(self, fab, *refs):
        src, out, theirs, mine, near, turn, last = refs if self.source is None else (self.source(), *refs)
        r, c = self.r, self.c
        rows = r // self.pieces
        half = rows // 2
        order = (6, 2, 4, 0)
        place = {0: 0, 2: 1, 4: 2, 6: 3}
        result = []

        def block(bits, at):
            slot = fab.slot(bits)
            if self.axis:
                return src.at[at, pl.ds(pl.multiple_of(slot * c, c), c)]
            return src.at[slot, at]

        for k in range(self.pieces):
            both = pl.ds(k * rows, rows)
            a, b = pl.ds(k * rows, half), pl.ds(k * rows + half, half)
            give = [fab.copy(block(s ^ 1, both), theirs.at[place[s], both], fab.partner) for s in order]
            load = [fab.here(block(s, both), mine.at[place[s], both]) for s in order]
            a0 = fab.copy(mine.at[3, a], near.at[1, a], fab.xn)
            a1 = fab.copy(mine.at[1, a], near.at[0, a], fab.xn)
            b0 = fab.copy(mine.at[3, b], near.at[1, b], fab.yn)
            b1 = fab.copy(mine.at[2, b], near.at[0, b], fab.yn)
            ta = fab.copy(turn.at[a], last.at[a], fab.yn)
            tb = fab.copy(turn.at[b], last.at[b], fab.xn)

            def begin(give=give, load=load):
                for g, h in zip(give, load, strict=True):
                    g.start()
                    h.start()

            def chip(k=k, give=give, load=load, both=both, a0=a0, a1=a1, b0=b0, b1=b1):
                for i, s in enumerate(order):
                    give[i].wait_recv()
                    load[i].wait()
                    q = place[s]
                    add_rows(mine.at[q, both], mine.at[q, both], theirs.at[q, both], rows)
                    if s == 6:
                        a0.start()
                        b0.start()
                    elif s == 2:
                        a1.start()
                    elif s == 4:
                        b1.start()

            def turn_a(a=a, a0=a0, ta=ta):
                a0.wait_recv()
                add_rows(turn.at[a], mine.at[2, a], near.at[1, a], half)
                ta.start()

            def turn_b(b=b, b0=b0, tb=tb):
                b0.wait_recv()
                add_rows(turn.at[b], mine.at[1, b], near.at[1, b], half)
                tb.start()

            def own(a=a, b=b, a1=a1, b1=b1, both=both):
                a1.wait_recv()
                b1.wait_recv()
                a1.wait_send()
                b1.wait_send()

            def close(a=a, b=b, give=give, a0=a0, b0=b0, ta=ta, tb=tb, both=both):
                ta.wait()
                tb.wait()
                step = math.gcd(rows, 16)

                def body(i, carry):
                    at = pl.ds(pl.multiple_of(i * step + both.start, step), step)
                    total = mine[0, at].astype(jnp.float32) + near[0, at].astype(jnp.float32)
                    out[at] = (total + last[at].astype(jnp.float32)).astype(out.dtype)
                    return carry

                lax.fori_loop(0, rows // step, body, 0)
                a0.wait_send()
                b0.wait_send()
                for g in give:
                    g.wait_send()

            t, s, w = self.at, self.span, self.wait
            result += [
                (t + k * 1e-3, begin),
                (t + 3 + w * 0.9 + k * s, chip),
                (t + w + 6 + (k + 0.7) * s, turn_a),
                (t + w + 6 + (k + 0.7) * s, turn_b),
                (t + w + 7 + (k + 0.9) * s, own),
                (t + w + 9 + (k + 1.3) * s, close),
            ]
        return result


class Line:
    def __init__(self, array, pieces=8, at=0.0, early=False):
        self.array, self.pieces, self.at, self.early = array, pieces, at, early
        self.arrays, self.outs = [array], [jax.ShapeDtypeStruct(array.shape, array.dtype)]
        self.in_spec = self.out_spec = VMEM
        self.scratch = [pltpu.VMEM(array.shape, array.dtype)] * 3
        self.sends, self.locals = 3 * pieces, 0
        self.load = 2 * array.size * array.dtype.itemsize / 80e3
        self.span = self.load / pieces

    def finish(self):
        return self.at + self.wait + self.load + 8.0

    def plain(self):
        return [lax.psum(self.array, "tensor")]

    def steps(self, fab, src, out, mixed, from_end, from_mid):
        inner = fab.inner
        rows = self.array.shape[0] // self.pieces
        result = []
        for k in range(self.pieces):
            at = pl.ds(k * rows, rows)
            up = fab.copy(src.at[at], from_end.at[at], fab.line)
            across = fab.copy(mixed.at[at], from_mid.at[at], fab.middle)
            down = fab.copy(out.at[at], out.at[at], fab.line)

            def begin(up=up):
                @pl.when(jnp.logical_not(inner))
                def _():
                    up.start()

            def meet(at=at, up=up, across=across):
                @pl.when(inner)
                def _():
                    up.wait_recv()
                    add_rows(mixed.at[at], src.at[at], from_end.at[at], rows)
                    across.start()

            def answer(at=at, across=across, down=down):
                @pl.when(inner)
                def _():
                    across.wait_recv()
                    add_rows(out.at[at], mixed.at[at], from_mid.at[at], rows)
                    down.start()

            def arrive(down=down):
                @pl.when(jnp.logical_not(inner))
                def _():
                    down.wait_recv()

            def end(up=up, across=across, down=down):
                @pl.when(inner)
                def _():
                    across.wait_send()
                    down.wait_send()

                @pl.when(jnp.logical_not(inner))
                def _():
                    up.wait_send()

            t, s, w = self.at, self.span, self.wait
            result += [
                (t, begin),
                (t + w + 2 + (k + 1) * s, meet),
                (t + w + 4 + (k + 2) * s, answer),
                (self.finish() if self.early else 1e8, arrive),
                (1e9, end),
            ]
        return result


def exchange(tasks, cid, fast):
    if not fast:
        return [out for task in tasks for out in task.plain()]
    lined = any(isinstance(task, (Line, Attend)) for task in tasks)
    planar = any(task.sends and not isinstance(task, (Line, Attend)) for task in tasks)
    swaps = any(isinstance(task, Swap) for task in tasks)
    busy = {True: 0.0, False: 0.0}
    for task in sorted(tasks, key=lambda each: each.at):
        task.wait = busy[isinstance(task, (Line, Attend))]
        if getattr(task, "source", None):
            task.wait = max(0.0, task.wait - task.at)
        busy[isinstance(task, (Line, Attend))] += task.load
    queue = [task for task in sorted(tasks, key=lambda each: each.at) if isinstance(task, (Gather, Swap))]
    for i, task in enumerate(queue):
        task.start = task.at
        if i > 1 and any(getattr(each, "early", False) for each in queue):
            task.start = max(task.at, queue[i - 2].at + queue[i - 2].wait + 2.1 + queue[i - 2].load * 2 / 3)
    given = sum(len(task.arrays) for task in tasks)
    made = sum(len(task.outs) for task in tasks)

    def kernel(*refs):
        ins, outs = list(refs[:given]), list(refs[given : given + made])
        send, recv, local = refs[-3:]
        scratch = list(refs[given + made : -3])
        fab = Fabric(send, recv, local)
        barrier = pltpu.get_barrier_semaphore()
        devices = []
        if swaps:
            devices = [(fab.slot(bits), fab.z) for bits in range(1, 8)]
        elif planar:
            devices = [fab.partner, fab.xn, fab.yn]
        if lined:
            devices.append(fab.line)
        for device in devices:
            pl.semaphore_signal(barrier, inc=1, device_id=device, device_id_type=MESH)
        if lined:

            @pl.when(fab.inner)
            def _():
                pl.semaphore_signal(barrier, inc=1, device_id=fab.middle, device_id_type=MESH)
                pl.semaphore_wait(barrier, len(devices) + 1)

            @pl.when(jnp.logical_not(fab.inner))
            def _():
                pl.semaphore_wait(barrier, len(devices))

        else:
            pl.semaphore_wait(barrier, len(devices))
        steps = []
        for task in tasks:
            own = [ins.pop(0) for _ in task.arrays]
            own += [outs.pop(0) for _ in task.outs]
            own += [scratch.pop(0) for _ in task.scratch]
            task.refs = own
        for task in tasks:
            steps += task.steps(fab, *task.refs)
        for _, step in sorted(steps, key=lambda pair: pair[0]):
            step()

    return pl.pallas_call(
        kernel,
        out_shape=[out for task in tasks for out in task.outs],
        in_specs=[spec for task in tasks for spec in (getattr(task, "in_specs", None) or [task.in_spec] * len(task.arrays))],
        out_specs=[task.out_spec for task in tasks for _ in task.outs],
        scratch_shapes=[s for task in tasks for s in task.scratch]
        + [
            pltpu.SemaphoreType.DMA((sum(task.sends for task in tasks),)),
            pltpu.SemaphoreType.DMA((sum(task.sends for task in tasks),)),
            pltpu.SemaphoreType.DMA((max(1, sum(task.locals for task in tasks)),)),
        ],
        compiler_params=pltpu.CompilerParams(collective_id=cid, has_side_effects=True, vmem_limit_bytes=63 * 1024 * 1024),
        name=f"exchange_{cid}",
    )(*[array for task in tasks for array in task.arrays])


def dot_nt(left, right):
    return lax.dot_general(left, right, (((1,), (1,)), ((), ())), preferred_element_type=jnp.float32)


def add_block(dst, first, second, rows):
    def body(i, carry):
        at = pl.ds(pl.multiple_of(i * 16, 16), 16)
        dst[at] = (first[at].astype(jnp.float32) + second[at].astype(jnp.float32)).astype(dst.dtype)
        return carry

    lax.fori_loop(0, rows // 16, body, 0)


def expert_stage(rows, mixing, upstream, gate, up, down, common_gate, common_up, common_down, cid):
    length, width = rows.shape
    pair = 2 * length
    units, common = gate.shape[1], common_gate.shape[1]
    segment, shared = lanes(units), lanes(common)
    wide = 2 * segment
    total = wide + shared
    both = 2 * total
    tile = 256
    low = rows.dtype
    half = width // 2
    full = width + 128
    cuts = (pl.ds(0, half), pl.ds(half, full - half))

    def kernel(
        x_h, mix_h, dy_h, wg_h, wu_h, wd_h, sg_h, su_h, sd_h,
        out_h, all_h, hm_h, dgu_h, own, own_mix,
        xs, mixs, dys, wg, wu, ws, wd, wc, dh, dgu, gs, us, ost, grads, theirs, near, turn, last,
        send, recv, local,
    ):
        fab = Fabric(send, recv, local)
        e = fab.e
        core = lax.rem(e, 2)
        mine = pl.ds(pl.multiple_of(core * length, length), length)
        other = pl.ds(pl.multiple_of((1 - core) * length, length), length)
        pairs = [fab.slot(bits) // 2 for bits in (0, 2, 4, 6)]

        barrier = pltpu.get_barrier_semaphore()
        for device in (fab.partner, fab.xn, fab.yn):
            pl.semaphore_signal(barrier, inc=1, device_id=device, device_id_type=MESH)
        pl.semaphore_wait(barrier, 3)

        quarter = length // 2

        def view(ref, bits, part=None):
            slot = fab.slot(bits)
            base = lax.rem(slot, 2) * length
            if part is None:
                return ref.at[slot // 2, pl.ds(pl.multiple_of(base, length), length)]
            return ref.at[slot // 2, pl.ds(pl.multiple_of(base + part * quarter, quarter), quarter)]

        def spread(src, ref):
            def forward(bits, device, part=None):
                return fab.copy(view(ref, bits, part), view(ref, bits, part), device)

            return {
                "load": fab.here(src, view(ref, 0)),
                "x": fab.copy(src, view(ref, 0), fab.xn),
                "y": fab.copy(src, view(ref, 0), fab.yn),
                "p": fab.copy(src, view(ref, 0), fab.partner),
                "lo": forward(2, fab.yn, 0),
                "hi": forward(4, fab.xn, 1),
                "px": forward(2, fab.partner),
                "py": forward(4, fab.partner),
                "plo": forward(6, fab.partner, 0),
                "phi": forward(6, fab.partner, 1),
            }

        moves = [spread(mix_h, mixs), spread(x_h, xs)]
        for name in ("x", "y", "p", "load"):
            for move in moves:
                move[name].start()
        def experts_of(src, dst):
            return [fab.here(src.at[i], dst.at[pl.ds(i * segment, units)]) for i in range(2)]

        def blocks_of(src, dst, first):
            d = src.shape[2]
            return [fab.here(src.at[j], dst.at[pl.ds(first, common), pl.ds(j * d, d)]) for j in range(src.shape[0])]

        load_out = experts_of(wd_h, wd) + blocks_of(sd_h, wc, 0)
        load_dy = [fab.here(dy_h.at[p], dys.at[p]) for p in pairs]
        load_in = experts_of(wg_h, wg) + experts_of(wu_h, wu) + blocks_of(sg_h, ws, 0) + blocks_of(su_h, ws, shared)
        for load in (*load_out, *load_dy, *load_in):
            load.start()
        for ref in (wd, wg, wu):
            for first in (units, segment + units):
                ref[first : first + segment - units, :] = jnp.zeros((segment - units, width), low)
        for ref, first in ((wc, common), (ws, common), (ws, shared + common)):
            ref[first : first + shared - common, :] = jnp.zeros((shared - common, width), low)
        keep = [fab.here(xs.at[p], all_h.at[p]) for p in pairs]
        keep_hm = [fab.here(dh.at[p], hm_h.at[p]) for p in pairs]
        keep_dgu = [fab.here(dgu, dgu_h.at[p]) for p in pairs]
        keep_out = [fab.here(ost.at[k % 2], out_h.at[p]) for k, p in enumerate(pairs)]

        give = [[fab.copy(grads.at[k, other, cut], theirs.at[k, :, cut], fab.partner) for cut in cuts] for k in range(4)]
        a, b = cuts
        a0 = fab.copy(grads.at[3, mine, a], near.at[1, :, a], fab.xn)
        a1 = fab.copy(grads.at[1, mine, a], near.at[0, :, a], fab.xn)
        b0 = fab.copy(grads.at[3, mine, b], near.at[1, :, b], fab.yn)
        b1 = fab.copy(grads.at[2, mine, b], near.at[0, :, b], fab.yn)
        ta = fab.copy(turn.at[:, a], last.at[:, a], fab.yn)
        tb = fab.copy(turn.at[:, b], last.at[:, b], fab.xn)

        def at_tile(n, first=0):
            return pl.ds(pl.multiple_of(first + n * tile, tile), tile)

        def back(p):
            def one(n, carry):
                at = at_tile(n)
                dh[p, :, at] = dot_nt(dys[p], wd[at, :]).astype(low)
                return carry

            lax.fori_loop(0, wide // tile, one, 0)
            dh[p, :, wide:total] = dot_nt(dys[p], wc[...]).astype(low)

        def hidden(p, k):
            def one(n, carry):
                at = at_tile(n)
                gs[:, at] = dot_nt(xs[p], wg[at, :])
                us[:, at] = dot_nt(xs[p], wu[at, :])
                return carry

            lax.fori_loop(0, wide // tile, one, 0)
            together = dot_nt(xs[p], ws[...])
            gs[:, wide:total] = together[:, :shared]
            us[:, wide:total] = together[:, shared:]

        def middle(p, k):
            step = 32

            def some(i, carry):
                at = pl.ds(pl.multiple_of(i * step, step), step)
                lane = lax.broadcasted_iota(jnp.int32, (step, 128), 1)
                expert = lax.rem(lane, 64)
                mixed = mixs[p, at].astype(jnp.float32)
                first = jnp.sum(jnp.where(expert == 2 * e, mixed, 0.0), axis=1, keepdims=True)
                second = jnp.sum(jnp.where(expert == 2 * e + 1, mixed, 0.0), axis=1, keepdims=True)

                def part(lo, hi, weight, to_gate, to_up):
                    gate, up = gs[at, lo:hi], us[at, lo:hi]
                    grad = dh[p, at, lo:hi].astype(jnp.float32)
                    logistic = sigmoid(gate)
                    active = gate * logistic
                    value = active * up
                    share = jnp.sum(value * grad, axis=1, keepdims=True)
                    grad = grad * weight
                    dh[p, at, lo:hi] = (value * weight).astype(low)
                    dgu[at, to_gate : to_gate + hi - lo] = (grad * up * (logistic + active * (1.0 - logistic))).astype(low)
                    dgu[at, to_up : to_up + hi - lo] = (grad * active).astype(low)
                    return share

                one = part(0, segment, first, 0, wide)
                two = part(segment, wide, second, segment, wide + segment)
                part(wide, total, 1.0, 2 * wide, 2 * wide + shared)
                shares = jnp.where(lane == 2 * e, one, jnp.where(lane == 2 * e + 1, two, 0.0))
                grads[k, at, width:full] = shares.astype(low)
                return carry

            lax.fori_loop(0, pair // step, some, 0)

        def inputs(p, k, first, count):
            def one(n, carry):
                at = at_tile(n, first)
                value = matmul(dgu[:, :wide], wg[:, at]) + matmul(dgu[:, wide : 2 * wide], wu[:, at])
                grads[k, :, at] = (value + matmul(dgu[:, 2 * wide :], ws[:, at])).astype(low)
                return carry

            lax.fori_loop(0, count // tile, one, 0)

        def outputs(p, k):
            if k > 1:
                keep_out[k - 2].wait()

            def one(n, carry):
                at = at_tile(n)
                value = matmul(dh[p, :, :wide], wd[:, at]) + matmul(dh[p, :, wide:], wc[:, at])
                ost[k % 2, :, at] = value.astype(low)
                return carry

            lax.fori_loop(0, width // tile, one, 0)
            keep_out[k].start()

        def compute(k):
            p = pairs[k]
            keep[k].start()
            hidden(p, k)
            if k > 0:
                keep_dgu[k - 1].wait()
            middle(p, k)
            keep_dgu[k].start()
            keep_hm[k].start()
            inputs(p, k, 0, half)
            give[k][0].start()
            inputs(p, k, half, half)
            give[k][1].start()

        def chip(k, part):
            give[k][part].wait_recv()
            cut = cuts[part]
            add_block(grads.at[k, mine, cut], grads.at[k, mine, cut], theirs.at[k, :, cut], length)

        for load in load_out:
            load.wait()
        for k in range(4):
            load_dy[k].wait()
            back(pairs[k])
        for load in load_in:
            load.wait()
        for move in moves:
            move["load"].wait()
            move["p"].wait_recv()
        compute(0)
        for move in moves:
            move["x"].wait_recv()
            move["lo"].start()
            move["px"].start()
        for move in moves:
            move["y"].wait_recv()
            move["hi"].start()
            move["py"].start()
        chip(0, 0)
        chip(0, 1)
        for move in moves:
            move["px"].wait_recv()
        compute(1)
        for move in moves:
            move["lo"].wait_recv()
            move["plo"].start()
            move["hi"].wait_recv()
            move["phi"].start()
        chip(1, 0)
        a1.start()
        chip(1, 1)
        for move in moves:
            move["py"].wait_recv()
        compute(2)
        chip(2, 1)
        b1.start()
        chip(2, 0)
        for move in moves:
            move["plo"].wait_recv()
            move["phi"].wait_recv()
        compute(3)
        chip(3, 0)
        a0.start()
        chip(3, 1)
        b0.start()
        outputs(pairs[0], 0)
        outputs(pairs[1], 1)
        outputs(pairs[2], 2)
        a0.wait_recv()
        add_block(turn.at[:, a], grads.at[2, mine, a], near.at[1, :, a], length)
        ta.start()
        b0.wait_recv()
        add_block(turn.at[:, b], grads.at[1, mine, b], near.at[1, :, b], length)
        tb.start()
        outputs(pairs[3], 3)
        a1.wait_recv()
        b1.wait_recv()
        ta.wait_recv()
        tb.wait_recv()

        def sum_up(i, carry):
            at = pl.ds(pl.multiple_of(i * 16, 16), 16)
            here = pl.ds(pl.multiple_of(core * length + i * 16, 16), 16)
            value = grads[0, here].astype(jnp.float32) + near[0, at].astype(jnp.float32)
            value = (value + last[at].astype(jnp.float32)).astype(low)
            own[at] = value[:, :width]
            own_mix[at] = value[:, width:]
            return carry

        lax.fori_loop(0, length // 16, sum_up, 0)
        for move in moves:
            for name in ("x", "y", "p", "lo", "hi", "px", "py", "plo", "phi"):
                move[name].wait_send()
        for k in range(4):
            for each in give[k]:
                each.wait_send()
            keep[k].wait()
            keep_hm[k].wait()
        keep_dgu[3].wait()
        keep_out[2].wait()
        keep_out[3].wait()
        for each in (a0, a1, b0, b1, ta, tb):
            each.wait_send()

    shape = jax.ShapeDtypeStruct
    vmem = pltpu.VMEM
    return pl.pallas_call(
        kernel,
        out_shape=[
            shape((4, pair, width), low),
            shape((4, pair, width), low),
            shape((4, pair, total), low),
            shape((4, pair, both), low),
            shape((length, width), low),
            shape((length, 128), low),
        ],
        in_specs=[ANY] * 9,
        out_specs=[ANY] * 4 + [VMEM] * 2,
        scratch_shapes=[
            vmem((4, pair, width), low),
            vmem((4, pair, 128), low),
            vmem((4, pair, width), low),
            vmem((wide, width), low),
            vmem((wide, width), low),
            vmem((2 * shared, width), low),
            vmem((wide, width), low),
            vmem((shared, width), low),
            vmem((4, pair, total), low),
            vmem((pair, both), low),
            vmem((pair, total), jnp.float32),
            vmem((pair, total), jnp.float32),
            vmem((2, pair, width), low),
            vmem((4, pair, full), low),
            vmem((4, length, full), low),
            vmem((2, length, full), low),
            vmem((length, full), low),
            vmem((length, full), low),
            pltpu.SemaphoreType.DMA((32,)),
            pltpu.SemaphoreType.DMA((32,)),
            pltpu.SemaphoreType.DMA((56,)),
        ],
        compiler_params=pltpu.CompilerParams(
            collective_id=cid, has_side_effects=True, vmem_limit_bytes=63 * 1024 * 1024
        ),
        name="expert_stage",
    )(rows, mixing, upstream.reshape(4, pair, width), gate, up, down, common_gate, common_up, common_down)


class Weights:
    sends, locals, load = 0, 80, 0.0

    def __init__(self, rows, grads, hidden, upstream, experts, units, common, own, at=0.0, pace=2.0):
        self.arrays = [rows, grads, hidden, upstream]
        self.in_spec = self.out_spec = ANY
        self.at, self.pace = at, pace
        self.tokens, self.width = rows.shape
        self.total = hidden.shape[1]
        self.experts, self.units, self.common, self.own = experts, units, common, own
        self.pad = lanes(units)
        self.wide = experts * self.pad
        self.shared = self.total - self.wide
        low = rows.dtype
        shape = jax.ShapeDtypeStruct
        whole, part = shape((experts, units, self.width), low), shape((self.width // own, common, own), low)
        self.outs = [whole, whole, whole, part, part, part]
        tile = pltpu.VMEM((2, experts, units, own), low)
        piece = pltpu.VMEM((2, common, own), low)
        self.scratch = [
            pltpu.VMEM(rows.shape, low),
            pltpu.VMEM(upstream.shape, low),
            pltpu.VMEM(hidden.shape, low),
            pltpu.VMEM(hidden.shape, low),
            pltpu.VMEM((self.total, self.tokens), low),
            pltpu.VMEM((2 * self.total, self.tokens), low),
            tile,
            tile,
            tile,
            piece,
            piece,
            piece,
        ]

    def plain(self):
        rows, grads, hidden, upstream = self.arrays
        low, wide, shared = rows.dtype, self.wide, self.shared
        into, out = matmul_tn(grads, rows).astype(low), matmul_tn(hidden, upstream).astype(low)

        def pick(array, first):
            return jnp.stack([array[first + i * self.pad :][: self.units] for i in range(self.experts)])

        def blocks(array, first):
            return array[first : first + self.common].reshape(self.common, -1, self.own).transpose(1, 0, 2)

        return [
            pick(into, 0),
            pick(into, wide),
            pick(out, 0),
            blocks(into, 2 * wide),
            blocks(into, 2 * wide + shared),
            blocks(out, wide),
        ]

    def steps(
        self, fab, x_h, g_h, h_h, y_h, gate_o, up_o, down_o, cg_o, cu_o, cd_o,
        xs, ys, s0, s1, ht, gt, gst, ust, dst, cgs, cus, cds,
    ):
        units, pad, wide, total, own, common = self.units, self.pad, self.wide, self.total, self.own, self.common
        columns = self.width // own
        load_h, load_y, load_x = fab.here(h_h, s0), fab.here(y_h, ys), fab.here(x_h, xs)
        load_lo = fab.here(g_h.at[:, pl.ds(0, total)], s1)
        load_hi = fab.here(g_h.at[:, pl.ds(total, total)], s0)

        def puts(n, whole, part):
            cols = pl.ds(n * own, own)
            copies = [fab.here(s.at[n % 2, i], o.at[i, :, cols]) for s, o in whole for i in range(self.experts)]
            return copies + [fab.here(s.at[n % 2], o.at[n]) for s, o in part]

        put_in = [puts(n, ((gst, gate_o), (ust, up_o)), ((cgs, cg_o), (cus, cu_o))) for n in range(columns)]
        put_out = [puts(n, ((dst, down_o),), ((cds, cd_o),)) for n in range(columns)]

        def begin():
            for each in (load_h, load_y, load_lo, load_x):
                each.start()

        def turn(dst_ref, src_ref, first):
            for at in range(0, total, 128):
                dst_ref[first + at : first + at + 128, :] = src_ref[:, at : at + 128].T

        def turn_hidden():
            load_h.wait()
            turn(ht, s0, 0)
            load_hi.start()

        def turn_lo():
            load_lo.wait()
            turn(gt, s1, 0)

        def turn_hi():
            load_hi.wait()
            turn(gt, s0, total)

        def store(stage, n, value):
            for i in range(self.experts):
                stage[n % 2, i] = value[i * pad : i * pad + units].astype(stage.dtype)

        def down(n):
            def step():
                if n == 0:
                    load_y.wait()
                if n >= 2:
                    for each in put_out[n - 2]:
                        each.wait()
                value = matmul(ht[...], ys[:, n * own : (n + 1) * own])
                store(dst, n, value)
                cds[n % 2] = value[wide : wide + common].astype(cds.dtype)
                for each in put_out[n]:
                    each.start()

            return step

        def gate(n):
            def step():
                if n == 0:
                    load_x.wait()
                if n >= 2:
                    for each in put_in[n - 2]:
                        each.wait()
                store(gst, n, matmul(gt[:wide], xs[:, n * own : (n + 1) * own]))

            return step

        def up(n):
            def step():
                value = matmul(gt[wide:], xs[:, n * own : (n + 1) * own])
                store(ust, n, value)
                cgs[n % 2] = value[wide : wide + common].astype(cgs.dtype)
                cus[n % 2] = value[wide + self.shared : wide + self.shared + common].astype(cus.dtype)
                for each in put_in[n]:
                    each.start()

            return step

        def end():
            for each in (*put_out[-2], *put_out[-1], *put_in[-2], *put_in[-1]):
                each.wait()

        t, p = self.at, self.pace
        result = [(t, begin), (t + 3, turn_hidden)]
        t += 4
        for n in range(columns):
            result.append((t, down(n)))
            t += 0.7 * p
        result.append((t, turn_lo))
        t += 0.7 * p
        result.append((t, turn_hi))
        t += 0.7 * p
        for n in range(columns):
            result.append((t, gate(n)))
            t += 0.6 * p
            result.append((t, up(n)))
            t += 0.8 * p
        result.append((1e9, end))
        return result


class Attend:
    names = ("sum", "normed", "query_nope", "query_rope", "latent_raw", "compressed", "key_rope", "expanded", "weights", "attended")

    def __init__(self, hidden, pre_gain, latent_gain, cosine, sine, segments, query, latent, expand, output, at=0.0):
        length = hidden.shape[0]
        self.heads = query.shape[1] // (HEAD_DIM + ROPE_DIM)
        self.at = at
        low = hidden.dtype
        shape = jax.ShapeDtypeStruct
        self.arrays = [
            hidden, pre_gain[None], latent_gain[None], cosine, sine, segments[:, None], segments[None],
            query, latent, expand, output,
        ]
        self.in_specs = [VMEM] * 7 + [ANY] * 4
        self.out_spec = VMEM
        heads = self.heads
        self.line = Line(shape(hidden.shape, low), at=at)
        self.outs = [
            shape(hidden.shape, low),
            shape(hidden.shape, low),
            shape((length, heads * HEAD_DIM), low),
            shape((length, heads * ROPE_DIM), low),
            shape((length, KV_RANK), jnp.float32),
            shape((length, KV_RANK), low),
            shape((length, ROPE_DIM), low),
            shape((length, heads * 2 * HEAD_DIM), low),
            shape((heads, length, length), jnp.float32),
            shape((length, heads * HEAD_DIM), low),
        ]
        self.scratch = [pltpu.VMEM(w.shape, low) for w in (query, latent, expand, output)]
        self.scratch += [pltpu.VMEM((length, query.shape[1]), jnp.float32), pltpu.VMEM(hidden.shape, low)] + self.line.scratch
        self.sends, self.locals, self.load = self.line.sends, 4, self.line.load

    def steps(
        self, fab, x, pre_gain, latent_gain, cos, sin, seg_col, seg_row, q_h, l_h, e_h, o_h,
        out, normed, q_nope, q_rope, raw, compressed, k_rope, expanded, probs, attended,
        wq, wl, we, wo, qs, part, mixed, from_end, from_mid,
    ):
        length = x.shape[0]
        loads = [fab.here(a, b) for a, b in ((l_h, wl), (q_h, wq), (e_h, we), (o_h, wo))]
        low = jnp.bfloat16
        scale = 1.0 / math.sqrt(HEAD_DIM + ROPE_DIM)

        def begin():
            for each in loads:
                each.start()

        def norm():
            def some(i, carry):
                at = pl.ds(pl.multiple_of(i * 32, 32), 32)
                v = x[at].astype(jnp.float32)
                inverse = lax.rsqrt(jnp.mean(v * v, axis=1, keepdims=True) + EPSILON)
                normed[at] = (v * inverse * pre_gain[...]).astype(low)
                return carry

            lax.fori_loop(0, length // 32, some, 0)

        def latent():
            loads[0].wait()
            every = dot_nt(normed[...], wl[...])
            value = every[:, :KV_RANK]
            raw[...] = value
            inverse = lax.rsqrt(jnp.mean(value * value, axis=1, keepdims=True) + EPSILON)
            compressed[...] = (value * inverse * latent_gain[...]).astype(low)
            k_rope[...] = rotate(every[:, KV_RANK:], cos[...], sin[...]).astype(low)

        def queries():
            loads[1].wait()

            def one(n, carry):
                at = pl.ds(pl.multiple_of(n * 256, 256), 256)
                qs[:, at] = matmul(normed[...], wq[:, at])
                return carry

            lax.fori_loop(0, qs.shape[1] // 256, one, 0)
            for h in range(self.heads):
                first = h * (HEAD_DIM + ROPE_DIM)
                q_nope[:, h * HEAD_DIM : (h + 1) * HEAD_DIM] = qs[:, first : first + HEAD_DIM].astype(low)
                turned = rotate(qs[:, first + HEAD_DIM : first + HEAD_DIM + ROPE_DIM], cos[...], sin[...])
                q_rope[:, h * ROPE_DIM : (h + 1) * ROPE_DIM] = turned.astype(low)

        def expand():
            loads[2].wait()
            for n in range(0, expanded.shape[1], 256):
                expanded[:, n : n + 256] = matmul(compressed[...], we[:, n : n + 256]).astype(low)

        def head(h):
            def step():
                first = 2 * HEAD_DIM * h
                scores = dot_nt(q_nope[:, h * HEAD_DIM : (h + 1) * HEAD_DIM], expanded[:, first : first + HEAD_DIM])
                scores = scores + dot_nt(q_rope[:, h * ROPE_DIM : (h + 1) * ROPE_DIM], k_rope[...])
                row = lax.broadcasted_iota(jnp.int32, (length, length), 0)
                column = lax.broadcasted_iota(jnp.int32, (length, length), 1)
                allowed = jnp.logical_and(column <= row, seg_col[...] == seg_row[...])
                scores = jnp.where(allowed, scores * scale, MASKED)
                raised = jnp.exp(scores - jnp.max(scores, axis=1, keepdims=True))
                chance = raised / jnp.sum(raised, axis=1, keepdims=True)
                probs[h] = chance
                value = matmul(chance.astype(low), expanded[:, first + HEAD_DIM : first + 2 * HEAD_DIM])
                attended[:, h * HEAD_DIM : (h + 1) * HEAD_DIM] = value.astype(low)

            return step

        def project():
            loads[3].wait()

            def one(n, carry):
                at = pl.ds(pl.multiple_of(n * 256, 256), 256)
                part[:, at] = matmul(attended[...], wo[:, at]).astype(low)
                return carry

            lax.fori_loop(0, part.shape[1] // 256, one, 0)

        t = self.at
        result = [(t, begin), (t + 0.1, norm), (t + 1, latent), (t + 3, queries), (t + 6, expand)]
        result += [(t + 7 + h, head(h)) for h in range(self.heads)]
        result.append((t + 12, project))
        self.line.at, self.line.wait = t + 14, 0.0
        return result + self.line.steps(fab, part, out, mixed, from_end, from_mid)


class Tail:
    sends, load = 0, 0.0

    def __init__(self, latent_line, normed_line, raw, latent_gain, normed, latent, hidden, pre_gain, grad_middle, small, at=0.0):
        self.at = at
        self.latent_line, self.normed_line = latent_line, normed_line
        self.arrays = [raw, latent_gain[None], normed, latent, hidden, pre_gain[None], grad_middle, small]
        self.in_spec = self.out_spec = VMEM
        low = hidden.dtype
        length, width = hidden.shape
        self.outs = [jax.ShapeDtypeStruct(hidden.shape, low)]
        depth = lanes(latent.shape[0])
        self.scratch = [
            pltpu.VMEM((length, depth), low),
            pltpu.VMEM((depth, length), low),
            pltpu.VMEM((latent.shape[0], width), low),
            pltpu.VMEM(small.shape, jnp.float32),
            pltpu.VMEM((length, width), jnp.float32),
            pltpu.VMEM((1, width), jnp.float32),
        ]
        self.locals = 1

    def latent_source(self):
        return self.refs[11]

    def small_source(self):
        return self.refs[12]

    def steps(self, fab, raw, latent_gain, normed, latent, hidden, pre_gain, grad_middle, small, out, gl, turned, lg, sm, gn, pre):
        latent_sum, normed_sum = self.latent_line.refs[1], self.normed_line.refs[1]
        length, width = hidden.shape
        rank = raw.shape[1]
        low = gl.dtype
        tile = 256

        def latent_back():
            grad, value = latent_sum[:, :rank].astype(jnp.float32), raw[...]
            inverse = lax.rsqrt(jnp.mean(value * value, axis=1, keepdims=True) + EPSILON)
            gain_grad = jnp.sum(grad * value * inverse, axis=0, keepdims=True)
            scaled = grad * latent_gain[...]
            inner = jnp.mean(scaled * value, axis=1, keepdims=True)
            gl[:, :rank] = (inverse * scaled - value * (inverse * inverse * inverse * inner)).astype(low)
            gl[:, rank:] = latent_sum[:, rank:]
            sm[...] = small[...]
            part = rank // 8
            for j in range(8):
                sm[j, 2:3, :part] = gain_grad[:, j * part : (j + 1) * part]
            for n in range(0, gl.shape[1], 128):
                turned[n : n + 128, :] = gl[:, n : n + 128].T

            def one(n, carry):
                at = pl.ds(pl.multiple_of(n * tile, tile), tile)
                lg[:, at] = matmul(turned[: lg.shape[0], :], normed[:, at]).astype(low)
                return carry

            lax.fori_loop(0, width // tile, one, 0)

        def normed_back():
            def one(n, carry):
                at = pl.ds(pl.multiple_of(n * tile, tile), tile)
                gn[:, at] = normed_sum[:, at].astype(jnp.float32) + matmul(gl[:, : latent.shape[0]], latent[:, at])
                return carry

            lax.fori_loop(0, width // tile, one, 0)
            pre[...] = jnp.zeros_like(pre)

            def some(i, carry):
                at = pl.ds(pl.multiple_of(i * 16, 16), 16)
                value, grad = hidden[at].astype(jnp.float32), gn[at]
                inverse = lax.rsqrt(jnp.mean(value * value, axis=1, keepdims=True) + EPSILON)
                pre[...] += jnp.sum(grad * value * inverse, axis=0, keepdims=True)
                scaled = grad * pre_gain[...]
                inner = jnp.mean(scaled * value, axis=1, keepdims=True)
                back = inverse * scaled - value * (inverse * inverse * inverse * inner)
                out[at] = (grad_middle[at] + back).astype(low)
                return carry

            lax.fori_loop(0, length // 16, some, 0)
            part = width // 8
            for j in range(8):
                sm[j, 0:1, :] = pre[:, j * part : (j + 1) * part]

        return [
            (self.latent_line.finish() + 0.1, latent_back),
            (self.normed_line.finish() + 0.1, normed_back),
        ]


def lanes(width):
    return -(-width // 128) * 128


def pad_to(array, axis, size):
    widths = [(0, 0)] * array.ndim
    widths[axis] = (0, size - array.shape[axis])
    return jnp.pad(array, widths) if widths[axis][1] else array


def shards(
    hidden_in,
    segment_ids,
    expert_ids,
    query_weight,
    latent_weight,
    expand_weight,
    output_weight,
    prenorm,
    latentnorm,
    postnorm,
    router_weight,
    shared_gate,
    shared_up,
    shared_down,
    expert_gate,
    expert_up,
    expert_down,
    cotangent,
):
    groups = lax.axis_size("expert")
    ranks = lax.axis_size("tensor")
    fast = groups == 8 and ranks == 4
    me = lax.axis_index("expert")
    local_experts, _, units = expert_gate.shape
    experts = local_experts * groups
    length = hidden_in.shape[0]
    tokens = groups * length
    own_d = prenorm.shape[0]
    own_latent = latentnorm.shape[0]
    common = shared_gate.shape[1] // groups
    unit_pad, common_pad = lanes(units), lanes(common)
    low = jnp.bfloat16

    small = jnp.concatenate(
        [
            prenorm[None],
            postnorm[None],
            pad_to(latentnorm[None], 1, own_d),
            jnp.zeros((5, own_d), low),
            router_weight.T,
        ],
        axis=0,
    )
    small_full, latent_full, query_full, expand_full, output_full = exchange(
        [
            Gather(small, at=0.0),
            Gather(latent_weight.T, axis=1, at=0.1),
            Gather(query_weight, at=0.2),
            Gather(expand_weight, at=0.3),
            Gather(output_weight, axis=1, at=0.4),
        ],
        0,
        fast,
    )
    query_full = query_full.reshape(D, -1)
    expand_full = expand_full.reshape(KV_RANK, -1)
    pre_gain = small_full[:, 0].reshape(D).astype(jnp.float32)
    post_gain = small_full[:, 1].reshape(D).astype(jnp.float32)
    latent_gain = small_full[:, 2, :own_latent].reshape(KV_RANK).astype(jnp.float32)
    router_full = small_full[:, 8:].transpose(1, 0, 2).reshape(experts, D)

    heads = query_full.shape[1] // (HEAD_DIM + ROPE_DIM)
    hidden = hidden_in.astype(jnp.float32)
    cosine, sine = rotary_tables(length)
    inverse_pre = lax.rsqrt(jnp.mean(hidden * hidden, axis=1, keepdims=True) + EPSILON)
    scale = 1.0 / math.sqrt(HEAD_DIM + ROPE_DIM)
    segments = segment_ids[0]

    def unit_blocks(weight):
        return weight.reshape(groups, common, own_d)

    beside = [
        Gather(cotangent, at=0.1),
        Swap(unit_blocks(shared_gate.T), at=0.2),
        Swap(unit_blocks(shared_up.T), at=0.3),
        Swap(unit_blocks(shared_down), at=0.4),
    ]
    if fast:
        attend = Attend(
            hidden_in, pre_gain, latent_gain, cosine, sine, segments, query_full, latent_full, expand_full, output_full,
            at=0.5,
        )
        (
            upstream_all,
            common_gate,
            common_up,
            common_down,
            attention,
            normed,
            query_nope,
            query_rope,
            latent_raw,
            compressed,
            key_rope,
            expanded,
            probabilities,
            attended,
        ) = exchange([*beside, attend], 1, fast)
    else:
        normed = (hidden * inverse_pre * pre_gain).astype(low)
        query_raw = matmul(normed, query_full).reshape(length, heads, HEAD_DIM + ROPE_DIM)
        query_nope = query_raw[:, :, :HEAD_DIM].astype(low)
        query_rope = rotate(query_raw[:, :, HEAD_DIM:], cosine[:, None, :], sine[:, None, :]).astype(low)
        latent_all = matmul_nt(normed, latent_full)
        latent_raw = latent_all[:, :KV_RANK]
        norm_latent = lax.rsqrt(jnp.mean(latent_raw * latent_raw, axis=1, keepdims=True) + EPSILON)
        compressed = (latent_raw * norm_latent * latent_gain).astype(low)
        key_rope = rotate(latent_all[:, KV_RANK:], cosine, sine).astype(low)
        expanded = matmul(compressed, expand_full).astype(low)
        parts = expanded.reshape(length, heads, 2 * HEAD_DIM)
        position = jnp.arange(length)
        allowed = (position[None, :] <= position[:, None]) & (segments[:, None] == segments[None, :])
        raw = jnp.einsum("qhd,khd->hqk", query_nope, parts[:, :, :HEAD_DIM], preferred_element_type=jnp.float32)
        raw = raw + jnp.einsum("qhr,kr->hqk", query_rope, key_rope, preferred_element_type=jnp.float32)
        scores = jnp.where(allowed[None], raw * scale, MASKED)
        raised = jnp.exp(scores - jnp.max(scores, axis=2, keepdims=True))
        probabilities = raised / jnp.sum(raised, axis=2, keepdims=True)
        attended = (
            jnp.einsum(
                "hqk,khd->qhd", probabilities.astype(low), parts[:, :, HEAD_DIM:], preferred_element_type=jnp.float32
            )
            .astype(low)
            .reshape(length, heads * HEAD_DIM)
        )
        upstream_all, common_gate, common_up, common_down, attention = exchange(
            [*beside, Line(matmul(attended, output_full).astype(low))], 1, fast
        )
    query_nope = query_nope.reshape(length, heads, HEAD_DIM)
    query_rope = query_rope.reshape(length, heads, ROPE_DIM)
    key_nope = expanded.reshape(length, heads, 2 * HEAD_DIM)[:, :, :HEAD_DIM]
    values = expanded.reshape(length, heads, 2 * HEAD_DIM)[:, :, HEAD_DIM:]
    probabilities_low = probabilities.astype(low)
    inverse_latent = lax.rsqrt(jnp.mean(latent_raw * latent_raw, axis=1, keepdims=True) + EPSILON)
    middle = hidden + attention.astype(jnp.float32)
    inverse_post = lax.rsqrt(jnp.mean(middle * middle, axis=1, keepdims=True) + EPSILON)
    normed_mid = (middle * inverse_post * post_gain).astype(low)
    affinity = sigmoid(matmul_nt(normed_mid, router_full))
    chosen = jnp.any(
        expert_ids[:, :, None] == jnp.arange(experts, dtype=jnp.int32)[None, None, :], axis=1
    ).astype(jnp.float32)
    selected = chosen * affinity
    selected_total = jnp.sum(selected, axis=1, keepdims=True)
    mixing = ROUTE_SCALE * selected / selected_total

    upstream_rows = upstream_all.reshape(tokens, D)
    gate_rows, up_rows = expert_gate.transpose(0, 2, 1), expert_up.transpose(0, 2, 1)
    wide = local_experts * unit_pad
    total = wide + common_pad
    if fast:
        high = mixing.astype(low)
        rest = (mixing - high.astype(jnp.float32)).astype(low)
        pair = jnp.concatenate([pad_to(high, 1, 64), pad_to(rest, 1, 64)], axis=1)
        mixture_rows, token_rows, mixed_hidden, grad_both, grad_own, mixing_grad_own = expert_stage(
            normed_mid,
            pair,
            upstream_all,
            gate_rows,
            up_rows,
            expert_down,
            common_gate,
            common_up,
            common_down,
            2,
        )
        token_rows = token_rows.reshape(tokens, D)
        mixed_hidden = mixed_hidden.reshape(tokens, total)
        grad_both = grad_both.reshape(tokens, 2 * total)
    else:
        token_rows = lax.all_gather(normed_mid, "expert", axis=0, tiled=True)
        mixing_own = lax.dynamic_slice_in_dim(
            lax.all_gather(mixing, "expert", axis=0, tiled=True), me * local_experts, local_experts, axis=1
        )
        segment = jnp.minimum(jnp.arange(total) // unit_pad, local_experts)
        scales = jnp.concatenate([mixing_own, jnp.ones((tokens, 1), jnp.float32)], axis=1)
        mixing_wide = sum(
            jnp.where(segment[None, :] == i, scales[:, i : i + 1], 0.0) for i in range(local_experts + 1)
        )

        def padded(weight):
            return jnp.concatenate([pad_to(weight[i], 0, unit_pad) for i in range(local_experts)], axis=0)

        def joined(blocks):
            return pad_to(blocks.transpose(1, 0, 2).reshape(common, D), 0, common_pad)

        weight_in = jnp.concatenate([padded(gate_rows), padded(up_rows), joined(common_gate), joined(common_up)], axis=0)
        weight_out = jnp.concatenate([padded(expert_down), joined(common_down)], axis=0)
        every = matmul_nt(token_rows, weight_in)
        gate = jnp.concatenate([every[:, :wide], every[:, 2 * wide : 2 * wide + common_pad]], axis=1)
        up = jnp.concatenate([every[:, wide : 2 * wide], every[:, 2 * wide + common_pad :]], axis=1)
        logistic = sigmoid(gate)
        unit_hidden = gate * logistic * up
        mixed_hidden = (unit_hidden * mixing_wide).astype(low)
        mixture_rows = matmul(mixed_hidden, weight_out).astype(low)
        grad_unit = matmul_nt(upstream_rows, weight_out)
        mixing_share = unit_hidden * grad_unit
        mixing_grad = jnp.stack(
            [jnp.sum(mixing_share[:, i * unit_pad : (i + 1) * unit_pad], axis=1) for i in range(local_experts)], axis=1
        )
        grad_hidden = grad_unit * mixing_wide
        grad_up = (grad_hidden * gate * logistic).astype(low)
        grad_gate = (grad_hidden * up * logistic * (1.0 + gate * (1.0 - logistic))).astype(low)
        grad_both = jnp.concatenate(
            [grad_gate[:, :wide], grad_up[:, :wide], grad_gate[:, wide:], grad_up[:, wide:]], axis=1
        )
        spread = jnp.arange(lanes(experts))
        mixing_grad_wide = sum(
            jnp.where(spread[None, :] == me * local_experts + i, mixing_grad[:, i : i + 1], 0.0)
            for i in range(local_experts)
        ).astype(low)
        grad_own = lax.psum_scatter(matmul(grad_both, weight_in).astype(low), "expert", tiled=True)
        mixing_grad_own = lax.psum_scatter(mixing_grad_wide, "expert", tiled=True)
    (
        grad_mid,
        grad_mixing,
        mixture_own,
        expert_gate_grad,
        expert_up_grad,
        expert_down_grad,
        common_gate_grad,
        common_up_grad,
        common_down_grad,
    ) = exchange(
        [
            Line(grad_own),
            Line(mixing_grad_own, pieces=1, at=-0.1),
            Scatter(mixture_rows.reshape(groups, length, D), pieces=4, at=0.2),
            Weights(
                token_rows, grad_both, mixed_hidden, upstream_rows, local_experts, units, common, own_d, at=1.0
            ),
        ],
        4,
        fast,
    )
    grad_mid = grad_mid.astype(jnp.float32)
    grad_mixing = grad_mixing[:, :experts].astype(jnp.float32)
    grad_selected = (
        ROUTE_SCALE
        * chosen
        * (
            grad_mixing / selected_total
            - jnp.sum(grad_mixing * selected, axis=1, keepdims=True) / (selected_total * selected_total)
        )
    )
    grad_logits = (grad_selected * affinity * (1.0 - affinity)).astype(low)
    router_grad = matmul_tn(grad_logits, normed_mid)
    grad_mid = grad_mid + matmul(grad_logits, router_full)
    upstream = cotangent.astype(jnp.float32)
    grad_middle_norm, post_grad = norm_backward(grad_mid, middle, inverse_post, post_gain)
    grad_middle = upstream + grad_middle_norm
    grad_attention = grad_middle.astype(low)
    output_grad = matmul_tn(attended, grad_attention)
    grad_attended = matmul_nt(grad_attention, output_full).astype(low).reshape(length, heads, HEAD_DIM)
    grad_probs = jnp.einsum("qhd,khd->hqk", grad_attended, values, preferred_element_type=jnp.float32)
    inner = jnp.sum(probabilities * grad_probs, axis=2, keepdims=True)
    grad_scores = (probabilities * (grad_probs - inner)).astype(low)
    grad_query_nope = scale * jnp.einsum("hqk,khd->qhd", grad_scores, key_nope, preferred_element_type=jnp.float32)
    grad_query_rope = scale * jnp.einsum("hqk,kr->qhr", grad_scores, key_rope, preferred_element_type=jnp.float32)
    grad_key_nope = scale * jnp.einsum("hqk,qhd->khd", grad_scores, query_nope, preferred_element_type=jnp.float32)
    grad_key_rope = scale * jnp.einsum("hqk,qhr->kr", grad_scores, query_rope, preferred_element_type=jnp.float32)
    grad_values = jnp.einsum("hqk,qhd->khd", probabilities_low, grad_attended, preferred_element_type=jnp.float32)
    grad_query = (
        jnp.concatenate(
            [grad_query_nope, rotate(grad_query_rope, cosine[:, None, :], -sine[:, None, :])], axis=2
        )
        .astype(low)
        .reshape(length, heads * (HEAD_DIM + ROPE_DIM))
    )
    query_grad = matmul_tn(normed, grad_query)
    grad_expanded = (
        jnp.concatenate([grad_key_nope, grad_values], axis=2).astype(low).reshape(length, heads * 2 * HEAD_DIM)
    )
    expand_grad = matmul_tn(compressed, grad_expanded)
    grad_key = pad_to(rotate(grad_key_rope, cosine, -sine), 1, lanes(ROPE_DIM))
    grad_latent_terms = jnp.concatenate([matmul_nt(grad_expanded, expand_full), grad_key], axis=1).astype(low)
    small_grad = jnp.concatenate(
        [
            jnp.zeros((groups, 1, own_d), jnp.float32),
            post_grad.reshape(groups, 1, own_d),
            jnp.zeros((groups, 14, own_d), jnp.float32),
            router_grad.reshape(experts, groups, own_d).transpose(1, 0, 2),
        ],
        axis=1,
    )
    latent_line = Line(grad_latent_terms, at=0.0, early=True)
    normed_line = Line(matmul_nt(grad_query, query_full).astype(low), at=0.05, early=True)
    dense = [
        Scatter(query_grad.astype(low).reshape(groups, own_d, -1), pieces=2, at=0.2),
        Scatter(expand_grad.astype(low).reshape(groups, own_latent, -1), at=0.4),
        Scatter(output_grad.astype(low), axis=1, pieces=2, at=0.6),
    ]
    swaps = [
        Swap(common_gate_grad, at=30.0),
        Swap(common_up_grad, at=30.1),
        Swap(common_down_grad, at=30.2),
    ]
    if fast:
        tail = Tail(
            latent_line, normed_line, latent_raw, latent_gain, normed, latent_full, hidden_in, pre_gain, grad_middle,
            small_grad,
        )
        shape = jax.ShapeDtypeStruct
        (
            _,
            _,
            query_out,
            expand_out,
            output_out,
            common_gate_out,
            common_up_out,
            common_down_out,
            mixture,
            latent_out,
            small_out,
            input_gradient,
        ) = exchange(
            [
                latent_line,
                normed_line,
                *dense,
                *swaps,
                Line(mixture_own, at=0.1),
                Scatter(shape((latent_full.shape[0], D), low), axis=1, pieces=2, at=24.0, source=tail.latent_source),
                Scatter(shape(small_grad.shape, jnp.float32), at=52.0, source=tail.small_source),
                tail,
            ],
            5,
            fast,
        )
    else:
        grad_latent_sum, grad_normed_sum, query_out, expand_out, output_out = exchange(
            [latent_line, normed_line, *dense], 5, fast
        )
        grad_latent_sum = grad_latent_sum.astype(jnp.float32)
        grad_latent_raw, latent_norm_grad = norm_backward(
            grad_latent_sum[:, :KV_RANK], latent_raw, inverse_latent, latent_gain
        )
        grad_latent = jnp.concatenate(
            [grad_latent_raw, grad_latent_sum[:, KV_RANK : KV_RANK + ROPE_DIM]], axis=1
        ).astype(low)
        latent_grad = matmul_tn(grad_latent, normed)
        grad_normed = grad_normed_sum.astype(jnp.float32) + matmul(grad_latent, latent_full)
        grad_hidden_in, pre_grad = norm_backward(grad_normed, hidden, inverse_pre, pre_gain)
        input_gradient = (grad_middle + grad_hidden_in).astype(low)
        small_grad = small_grad.at[:, 0].set(pre_grad.reshape(groups, own_d))
        small_grad = small_grad.at[:, 2, :own_latent].set(latent_norm_grad.reshape(groups, own_latent))
        mixture, latent_out, small_out, common_gate_out, common_up_out, common_down_out = exchange(
            [
                Line(mixture_own),
                Scatter(latent_grad.astype(low), axis=1, pieces=2, at=0.2),
                Scatter(small_grad, at=0.1),
                *swaps,
            ],
            6,
            fast,
        )
    block_output = (middle + mixture.astype(jnp.float32)).astype(low)

    def unit_rows(back):
        return back.reshape(groups * common, own_d).astype(jnp.float32)

    return (
        block_output,
        input_gradient,
        query_out.astype(jnp.float32),
        latent_out.T.astype(jnp.float32),
        expand_out.astype(jnp.float32),
        output_out.astype(jnp.float32),
        small_out[0],
        small_out[2, :own_latent],
        small_out[1],
        small_out[16:].T,
        unit_rows(common_gate_out).T,
        unit_rows(common_up_out).T,
        unit_rows(common_down_out),
        expert_gate_grad.astype(jnp.float32).transpose(0, 2, 1),
        expert_up_grad.astype(jnp.float32).transpose(0, 2, 1),
        expert_down_grad.astype(jnp.float32),
    )


def solution(mesh):
    placed = (
        P("expert", None),
        P("expert", None),
        P("expert", None),
        P("expert", "tensor"),
        P("expert", None),
        P("expert", "tensor"),
        P("tensor", "expert"),
        P("expert"),
        P("expert"),
        P("expert"),
        P("expert", None),
        P("expert", "tensor"),
        P("expert", "tensor"),
        P("tensor", "expert"),
        P("expert", None, "tensor"),
        P("expert", None, "tensor"),
        P("expert", "tensor", None),
        P("expert", None),
    )
    return jax.shard_map(
        shards,
        mesh=mesh,
        in_specs=placed,
        out_specs=(
            P("expert", None),
            P("expert", None),
            P("expert", "tensor"),
            P("expert", None),
            P("expert", "tensor"),
            P("tensor", "expert"),
            P("expert"),
            P("expert"),
            P("expert"),
            P("expert", None),
            P("expert", "tensor"),
            P("expert", "tensor"),
            P("tensor", "expert"),
            P("expert", None, "tensor"),
            P("expert", None, "tensor"),
            P("expert", "tensor", None),
        ),
        check_vma=False,
    )
```

```python
import math

import jax
import jax.numpy as jnp
from jax import lax
from jax.experimental import pallas as pl
from jax.experimental.pallas import tpu as pltpu
from jax.sharding import PartitionSpec as P

D = 2048
HEAD_DIM = 128
ROPE_DIM = 64
KV_RANK = 512
TOP = 6


EPSILON = 1e-06
ROUTE_SCALE = 2.446
ROPE_BASE = 50000.0
MASKED = -1e30


def matmul(left, right):
    return jnp.dot(left, right, preferred_element_type=jnp.float32)


def matmul_nt(left, right):
    return lax.dot_general(
        left, right, (((1,), (1,)), ((), ())), preferred_element_type=jnp.float32
    )


def matmul_tn(left, right):
    return lax.dot_general(
        left, right, (((0,), (0,)), ((), ())), preferred_element_type=jnp.float32
    )


def rotary_tables(length):
    position = jnp.arange(length).astype(jnp.float32)
    exponent = jnp.arange(ROPE_DIM // 2).astype(jnp.float32) * (2.0 / ROPE_DIM)
    angles = position[:, None] * jnp.exp(-math.log(ROPE_BASE) * exponent)[None, :]
    return (jnp.cos(angles), jnp.sin(angles))


def rotate(values, cosine, sine):
    half = values.shape[-1] // 2
    first = values[..., :half]
    second = values[..., half:]
    return jnp.concatenate(
        [first * cosine - second * sine, second * cosine + first * sine], axis=-1
    )


def sigmoid(values):
    return 1.0 / (1.0 + jnp.exp(-values))


def norm_backward(grad_normed, values, inverse, gain):
    gain_grad = jnp.sum(grad_normed * values * inverse, axis=0)
    scaled = grad_normed * gain
    inner = jnp.mean(scaled * values, axis=1, keepdims=True)
    return (inverse * scaled - values * inverse * inverse * inverse * inner, gain_grad)


MESH = pl.DeviceIdType.MESH
ANY = pl.BlockSpec(memory_space=pl.ANY)
VMEM = pl.BlockSpec(memory_space=pltpu.VMEM)


def xor_bit(value, bit):
    return value + bit - 2 * bit * lax.rem(value // bit, 2)


def add_rows(dst, first, second, rows):
    step = math.gcd(rows, 16)

    def body(i, carry):
        at = pl.ds(pl.multiple_of(i * step, step), step)
        total = first[at].astype(jnp.float32) + second[at].astype(jnp.float32)
        dst[at] = total.astype(dst.dtype)
        return carry

    lax.fori_loop(0, rows // step, body, 0)


class Fabric:
    def __init__(self, send, recv, local):
        self.send, self.recv, self.local = send, recv, local
        self.used = self.local_used = 0
        self.e = lax.axis_index("expert")
        self.z = lax.axis_index("tensor")
        self.partner = (xor_bit(self.e, 1), self.z)
        self.xn = (xor_bit(self.e, 2), self.z)
        self.yn = (xor_bit(self.e, 4), self.z)
        self.line = (self.e, xor_bit(self.z, 1))
        self.middle = (self.e, 3 - self.z)
        self.inner = jnp.logical_or(self.z == 1, self.z == 2)

    def copy(self, src, dst, device):
        k = self.used
        self.used += 1
        return pltpu.make_async_remote_copy(
            src_ref=src,
            dst_ref=dst,
            send_sem=self.send.at[k],
            recv_sem=self.recv.at[k],
            device_id=device,
            device_id_type=MESH,
        )

    def here(self, src, dst):
        k = self.local_used
        self.local_used += 1
        return pltpu.make_async_copy(src, dst, self.local.at[k])

    def slot(self, bits):
        e = self.e
        for bit in (1, 2, 4):
            if bits & bit:
                e = xor_bit(e, bit)
        return e


class Gather:
    sends, locals = 9, 2

    def __init__(self, array, axis=0, at=0.0, early=False):
        self.array, self.axis, self.at, self.early = array, axis, at, early
        r, c = array.shape
        shape = (r, 8 * c) if axis else (8, r, c)
        self.arrays, self.outs = [array], [jax.ShapeDtypeStruct(shape, array.dtype)]
        self.in_spec = self.out_spec = ANY
        self.scratch = [pltpu.VMEM(array.shape, array.dtype)]
        self.span = self.load = 3 * 2 * array.size * array.dtype.itemsize / 160e3

    def finish(self):
        return self.at + self.wait + self.load + 5.0

    def plain(self):
        return [lax.all_gather(self.array, "expert", axis=self.axis, tiled=bool(self.axis))]

    def steps(self, fab, src, dst, held):
        r, c = self.array.shape
        h = (r // 2 + 15) // 16 * 16 if r > 16 else r // 2
        parts = {0: pl.ds(0, h), 1: pl.ds(h, r - h), None: pl.ds(0, r)}

        def view(bits, part=None):
            slot = fab.slot(bits)
            if self.axis:
                return dst.at[parts[part], pl.ds(pl.multiple_of(slot * c, c), c)]
            return dst.at[slot, parts[part]]

        def forward(bits, device, part=None):
            return fab.copy(view(bits, part), view(bits, part), device)

        load, store = fab.here(src, held), fab.here(held, view(0))
        to_x, to_y, to_p = (fab.copy(src, view(0), d) for d in (fab.xn, fab.yn, fab.partner))
        lo, hi = forward(2, fab.yn, 0), forward(4, fab.xn, 1)
        px, py = forward(2, fab.partner), forward(4, fab.partner)
        plo, phi = forward(6, fab.partner, 0), forward(6, fab.partner, 1)

        def begin():
            for each in (to_x, to_y, to_p, load):
                each.start()

        def keep():
            load.wait()
            store.start()

        def from_x():
            to_x.wait_recv()
            lo.start()
            px.start()

        def from_y():
            to_y.wait_recv()
            hi.start()
            py.start()

        def corner_lo():
            lo.wait_recv()
            plo.start()

        def corner_hi():
            hi.wait_recv()
            phi.start()

        def arrive():
            store.wait()
            for each in (to_p, px, py, plo, phi):
                each.wait_recv()

        def end():
            for each in (to_x, to_y, to_p, lo, hi, px, py, plo, phi):
                each.wait_send()

        t, s, w = self.at, self.span, self.wait
        return [
            (self.start, begin),
            (self.start + 2, keep),
            (t + w + 2 + s * 2 / 3, from_x),
            (t + w + 2 + s * 2 / 3, from_y),
            (t + w + 3 + s, corner_lo),
            (t + w + 3 + s, corner_hi),
            (self.finish() if self.early else 1e8, arrive),
            (1e9, end),
        ]


class Swap:
    sends, locals = 7, 2

    def __init__(self, array, at=0.0):
        self.array, self.at = array, at
        self.arrays, self.outs = [array], [jax.ShapeDtypeStruct(array.shape, array.dtype)]
        self.in_spec = self.out_spec = ANY
        self.scratch = [pltpu.VMEM(array.shape[1:], array.dtype)]
        self.load = array.size * array.dtype.itemsize / 80e3

    def plain(self):
        return [lax.all_to_all(self.array, "expert", split_axis=0, concat_axis=0, tiled=True)]

    def steps(self, fab, src, dst, held):
        e = fab.e
        load, store = fab.here(src.at[e], held), fab.here(held, dst.at[e])
        copies = []
        for bits in (6, 7, 2, 3, 4, 5, 1):
            other = fab.slot(bits)
            copies.append(fab.copy(src.at[other], dst.at[e], (other, fab.z)))

        def begin():
            for each in copies:
                each.start()
            load.start()

        def keep():
            load.wait()
            store.start()

        def end():
            store.wait()
            for each in copies:
                each.wait()

        return [(self.start, begin), (self.start + 2, keep), (1e9, end)]


class Scatter:
    def __init__(self, array, axis=0, pieces=1, at=0.0, out_dtype=None, source=None):
        self.array, self.axis, self.pieces, self.at, self.source = array, axis, pieces, at, source
        if axis:
            r, c = array.shape[0], array.shape[1] // 8
        else:
            r, c = array.shape[1:]
        self.r, self.c = r, c
        self.arrays, self.outs = [array], [jax.ShapeDtypeStruct((r, c), out_dtype or array.dtype)]
        if source:
            self.arrays = []
        self.in_spec, self.out_spec = ANY, VMEM
        d = array.dtype
        self.scratch = [
            pltpu.VMEM((4, r, c), d),
            pltpu.VMEM((4, r, c), d),
            pltpu.VMEM((2, r, c), d),
            pltpu.VMEM((r, c), d),
            pltpu.VMEM((r, c), d),
        ]
        self.sends, self.locals = 10 * pieces, 4 * pieces
        self.load = 3 * 2 * r * c * d.itemsize / 160e3
        self.span = self.load / pieces

    def plain(self):
        if self.axis:
            out = lax.psum_scatter(self.array, "expert", scatter_dimension=1, tiled=True)
        else:
            out = lax.psum_scatter(self.array, "expert", scatter_dimension=0, tiled=False)
        return [out.astype(self.outs[0].dtype)]

    def steps(self, fab, *refs):
        src, out, theirs, mine, near, turn, last = refs if self.source is None else (self.source(), *refs)
        r, c = self.r, self.c
        rows = r // self.pieces
        half = rows // 2
        order = (6, 2, 4, 0)
        place = {0: 0, 2: 1, 4: 2, 6: 3}
        result = []

        def block(bits, at):
            slot = fab.slot(bits)
            if self.axis:
                return src.at[at, pl.ds(pl.multiple_of(slot * c, c), c)]
            return src.at[slot, at]

        for k in range(self.pieces):
            both = pl.ds(k * rows, rows)
            a, b = pl.ds(k * rows, half), pl.ds(k * rows + half, half)
            give = [fab.copy(block(s ^ 1, both), theirs.at[place[s], both], fab.partner) for s in order]
            load = [fab.here(block(s, both), mine.at[place[s], both]) for s in order]
            a0 = fab.copy(mine.at[3, a], near.at[1, a], fab.xn)
            a1 = fab.copy(mine.at[1, a], near.at[0, a], fab.xn)
            b0 = fab.copy(mine.at[3, b], near.at[1, b], fab.yn)
            b1 = fab.copy(mine.at[2, b], near.at[0, b], fab.yn)
            ta = fab.copy(turn.at[a], last.at[a], fab.yn)
            tb = fab.copy(turn.at[b], last.at[b], fab.xn)

            def begin(give=give, load=load):
                for g, h in zip(give, load, strict=True):
                    g.start()
                    h.start()

            def chip(k=k, give=give, load=load, both=both, a0=a0, a1=a1, b0=b0, b1=b1):
                for i, s in enumerate(order):
                    give[i].wait_recv()
                    load[i].wait()
                    q = place[s]
                    add_rows(mine.at[q, both], mine.at[q, both], theirs.at[q, both], rows)
                    if s == 6:
                        a0.start()
                        b0.start()
                    elif s == 2:
                        a1.start()
                    elif s == 4:
                        b1.start()

            def turn_a(a=a, a0=a0, ta=ta):
                a0.wait_recv()
                add_rows(turn.at[a], mine.at[2, a], near.at[1, a], half)
                ta.start()

            def turn_b(b=b, b0=b0, tb=tb):
                b0.wait_recv()
                add_rows(turn.at[b], mine.at[1, b], near.at[1, b], half)
                tb.start()

            def own(a=a, b=b, a1=a1, b1=b1, both=both):
                a1.wait_recv()
                b1.wait_recv()
                a1.wait_send()
                b1.wait_send()

            def close(a=a, b=b, give=give, a0=a0, b0=b0, ta=ta, tb=tb, both=both):
                ta.wait()
                tb.wait()
                step = math.gcd(rows, 16)

                def body(i, carry):
                    at = pl.ds(pl.multiple_of(i * step + both.start, step), step)
                    total = mine[0, at].astype(jnp.float32) + near[0, at].astype(jnp.float32)
                    out[at] = (total + last[at].astype(jnp.float32)).astype(out.dtype)
                    return carry

                lax.fori_loop(0, rows // step, body, 0)
                a0.wait_send()
                b0.wait_send()
                for g in give:
                    g.wait_send()

            t, s, w = self.at, self.span, self.wait
            result += [
                (t + k * 1e-3, begin),
                (t + 3 + w * 0.9 + k * s, chip),
                (t + w + 6 + (k + 0.7) * s, turn_a),
                (t + w + 6 + (k + 0.7) * s, turn_b),
                (t + w + 7 + (k + 0.9) * s, own),
                (t + w + 9 + (k + 1.3) * s, close),
            ]
        return result


class Line:
    def __init__(self, array, pieces=8, at=0.0, early=False):
        self.array, self.pieces, self.at, self.early = array, pieces, at, early
        self.arrays, self.outs = [array], [jax.ShapeDtypeStruct(array.shape, array.dtype)]
        self.in_spec = self.out_spec = VMEM
        self.scratch = [pltpu.VMEM(array.shape, array.dtype)] * 3
        self.sends, self.locals = 3 * pieces, 0
        self.load = 2 * array.size * array.dtype.itemsize / 80e3
        self.span = self.load / pieces

    def finish(self):
        return self.at + self.wait + self.load + 8.0

    def plain(self):
        return [lax.psum(self.array, "tensor")]

    def steps(self, fab, src, out, mixed, from_end, from_mid):
        inner = fab.inner
        rows = self.array.shape[0] // self.pieces
        result = []
        for k in range(self.pieces):
            at = pl.ds(k * rows, rows)
            up = fab.copy(src.at[at], from_end.at[at], fab.line)
            across = fab.copy(mixed.at[at], from_mid.at[at], fab.middle)
            down = fab.copy(out.at[at], out.at[at], fab.line)

            def begin(up=up):
                @pl.when(jnp.logical_not(inner))
                def _():
                    up.start()

            def meet(at=at, up=up, across=across):
                @pl.when(inner)
                def _():
                    up.wait_recv()
                    add_rows(mixed.at[at], src.at[at], from_end.at[at], rows)
                    across.start()

            def answer(at=at, across=across, down=down):
                @pl.when(inner)
                def _():
                    across.wait_recv()
                    add_rows(out.at[at], mixed.at[at], from_mid.at[at], rows)
                    down.start()

            def arrive(down=down):
                @pl.when(jnp.logical_not(inner))
                def _():
                    down.wait_recv()

            def end(up=up, across=across, down=down):
                @pl.when(inner)
                def _():
                    across.wait_send()
                    down.wait_send()

                @pl.when(jnp.logical_not(inner))
                def _():
                    up.wait_send()

            t, s, w = self.at, self.span, self.wait
            result += [
                (t, begin),
                (t + w + 2 + (k + 1) * s, meet),
                (t + w + 4 + (k + 2) * s, answer),
                (self.finish() if self.early else 1e8, arrive),
                (1e9, end),
            ]
        return result


def exchange(tasks, cid, fast):
    if not fast:
        return [out for task in tasks for out in task.plain()]
    lined = any(isinstance(task, (Line, Attend)) for task in tasks)
    planar = any(task.sends and not isinstance(task, (Line, Attend)) for task in tasks)
    swaps = any(isinstance(task, Swap) for task in tasks)
    busy = {True: 0.0, False: 0.0}
    for task in sorted(tasks, key=lambda each: each.at):
        task.wait = busy[isinstance(task, (Line, Attend))]
        if getattr(task, "source", None):
            task.wait = max(0.0, task.wait - task.at)
        busy[isinstance(task, (Line, Attend))] += task.load
    queue = [task for task in sorted(tasks, key=lambda each: each.at) if isinstance(task, (Gather, Swap))]
    for i, task in enumerate(queue):
        task.start = task.at
        if i > 1 and any(getattr(each, "early", False) for each in queue):
            task.start = max(task.at, queue[i - 2].at + queue[i - 2].wait + 2.1 + queue[i - 2].load * 2 / 3)
    given = sum(len(task.arrays) for task in tasks)
    made = sum(len(task.outs) for task in tasks)

    def kernel(*refs):
        ins, outs = list(refs[:given]), list(refs[given : given + made])
        send, recv, local = refs[-3:]
        scratch = list(refs[given + made : -3])
        fab = Fabric(send, recv, local)
        barrier = pltpu.get_barrier_semaphore()
        devices = []
        if swaps:
            devices = [(fab.slot(bits), fab.z) for bits in range(1, 8)]
        elif planar:
            devices = [fab.partner, fab.xn, fab.yn]
        if lined:
            devices.append(fab.line)
        for device in devices:
            pl.semaphore_signal(barrier, inc=1, device_id=device, device_id_type=MESH)
        if lined:

            @pl.when(fab.inner)
            def _():
                pl.semaphore_signal(barrier, inc=1, device_id=fab.middle, device_id_type=MESH)
                pl.semaphore_wait(barrier, len(devices) + 1)

            @pl.when(jnp.logical_not(fab.inner))
            def _():
                pl.semaphore_wait(barrier, len(devices))

        else:
            pl.semaphore_wait(barrier, len(devices))
        steps = []
        for task in tasks:
            own = [ins.pop(0) for _ in task.arrays]
            own += [outs.pop(0) for _ in task.outs]
            own += [scratch.pop(0) for _ in task.scratch]
            task.refs = own
        for task in tasks:
            steps += task.steps(fab, *task.refs)
        for _, step in sorted(steps, key=lambda pair: pair[0]):
            step()

    return pl.pallas_call(
        kernel,
        out_shape=[out for task in tasks for out in task.outs],
        in_specs=[spec for task in tasks for spec in (getattr(task, "in_specs", None) or [task.in_spec] * len(task.arrays))],
        out_specs=[task.out_spec for task in tasks for _ in task.outs],
        scratch_shapes=[s for task in tasks for s in task.scratch]
        + [
            pltpu.SemaphoreType.DMA((sum(task.sends for task in tasks),)),
            pltpu.SemaphoreType.DMA((sum(task.sends for task in tasks),)),
            pltpu.SemaphoreType.DMA((max(1, sum(task.locals for task in tasks)),)),
        ],
        compiler_params=pltpu.CompilerParams(collective_id=cid, has_side_effects=True, vmem_limit_bytes=63 * 1024 * 1024),
        name=f"exchange_{cid}",
    )(*[array for task in tasks for array in task.arrays])


def dot_nt(left, right):
    return lax.dot_general(left, right, (((1,), (1,)), ((), ())), preferred_element_type=jnp.float32)


def add_block(dst, first, second, rows):
    def body(i, carry):
        at = pl.ds(pl.multiple_of(i * 16, 16), 16)
        dst[at] = (first[at].astype(jnp.float32) + second[at].astype(jnp.float32)).astype(dst.dtype)
        return carry

    lax.fori_loop(0, rows // 16, body, 0)


def expert_stage(rows, mixing, upstream, gate, up, down, common_gate, common_up, common_down, cid):
    length, width = rows.shape
    pair = 2 * length
    units, common = gate.shape[1], common_gate.shape[1]
    segment, shared = lanes(units), lanes(common)
    wide = 2 * segment
    total = wide + shared
    both = 2 * total
    tile = 256
    low = rows.dtype
    half = width // 2
    full = width + 128
    cuts = (pl.ds(0, half), pl.ds(half, full - half))

    def kernel(
        x_h, mix_h, dy_h, wg_h, wu_h, wd_h, sg_h, su_h, sd_h,
        out_h, all_h, hm_h, dgu_h, own, own_mix,
        xs, mixs, dys, wg, wu, ws, wd, wc, dh, dgu, gs, us, ost, grads, theirs, near, turn, last,
        send, recv, local,
    ):
        fab = Fabric(send, recv, local)
        e = fab.e
        core = lax.rem(e, 2)
        mine = pl.ds(pl.multiple_of(core * length, length), length)
        other = pl.ds(pl.multiple_of((1 - core) * length, length), length)
        pairs = [fab.slot(bits) // 2 for bits in (0, 2, 4, 6)]

        barrier = pltpu.get_barrier_semaphore()
        for device in (fab.partner, fab.xn, fab.yn):
            pl.semaphore_signal(barrier, inc=1, device_id=device, device_id_type=MESH)
        pl.semaphore_wait(barrier, 3)

        quarter = length // 2

        def view(ref, bits, part=None):
            slot = fab.slot(bits)
            base = lax.rem(slot, 2) * length
            if part is None:
                return ref.at[slot // 2, pl.ds(pl.multiple_of(base, length), length)]
            return ref.at[slot // 2, pl.ds(pl.multiple_of(base + part * quarter, quarter), quarter)]

        def spread(src, ref):
            def forward(bits, device, part=None):
                return fab.copy(view(ref, bits, part), view(ref, bits, part), device)

            return {
                "load": fab.here(src, view(ref, 0)),
                "x": fab.copy(src, view(ref, 0), fab.xn),
                "y": fab.copy(src, view(ref, 0), fab.yn),
                "p": fab.copy(src, view(ref, 0), fab.partner),
                "lo": forward(2, fab.yn, 0),
                "hi": forward(4, fab.xn, 1),
                "px": forward(2, fab.partner),
                "py": forward(4, fab.partner),
                "plo": forward(6, fab.partner, 0),
                "phi": forward(6, fab.partner, 1),
            }

        moves = [spread(mix_h, mixs), spread(x_h, xs)]
        for name in ("x", "y", "p", "load"):
            for move in moves:
                move[name].start()
        def experts_of(src, dst):
            return [fab.here(src.at[i], dst.at[pl.ds(i * segment, units)]) for i in range(2)]

        def blocks_of(src, dst, first):
            d = src.shape[2]
            return [fab.here(src.at[j], dst.at[pl.ds(first, common), pl.ds(j * d, d)]) for j in range(src.shape[0])]

        load_out = experts_of(wd_h, wd) + blocks_of(sd_h, wc, 0)
        load_dy = [fab.here(dy_h.at[p], dys.at[p]) for p in pairs]
        load_in = experts_of(wg_h, wg) + experts_of(wu_h, wu) + blocks_of(sg_h, ws, 0) + blocks_of(su_h, ws, shared)
        for load in (*load_out, *load_dy, *load_in):
            load.start()
        for ref in (wd, wg, wu):
            for first in (units, segment + units):
                ref[first : first + segment - units, :] = jnp.zeros((segment - units, width), low)
        for ref, first in ((wc, common), (ws, common), (ws, shared + common)):
            ref[first : first + shared - common, :] = jnp.zeros((shared - common, width), low)
        keep = [fab.here(xs.at[p], all_h.at[p]) for p in pairs]
        keep_hm = [fab.here(dh.at[p], hm_h.at[p]) for p in pairs]
        keep_dgu = [fab.here(dgu, dgu_h.at[p]) for p in pairs]
        keep_out = [fab.here(ost.at[k % 2], out_h.at[p]) for k, p in enumerate(pairs)]

        give = [[fab.copy(grads.at[k, other, cut], theirs.at[k, :, cut], fab.partner) for cut in cuts] for k in range(4)]
        a, b = cuts
        a0 = fab.copy(grads.at[3, mine, a], near.at[1, :, a], fab.xn)
        a1 = fab.copy(grads.at[1, mine, a], near.at[0, :, a], fab.xn)
        b0 = fab.copy(grads.at[3, mine, b], near.at[1, :, b], fab.yn)
        b1 = fab.copy(grads.at[2, mine, b], near.at[0, :, b], fab.yn)
        ta = fab.copy(turn.at[:, a], last.at[:, a], fab.yn)
        tb = fab.copy(turn.at[:, b], last.at[:, b], fab.xn)

        def at_tile(n, first=0):
            return pl.ds(pl.multiple_of(first + n * tile, tile), tile)

        def back(p):
            def one(n, carry):
                at = at_tile(n)
                dh[p, :, at] = dot_nt(dys[p], wd[at, :]).astype(low)
                return carry

            lax.fori_loop(0, wide // tile, one, 0)
            dh[p, :, wide:total] = dot_nt(dys[p], wc[...]).astype(low)

        def hidden(p, k):
            def one(n, carry):
                at = at_tile(n)
                gs[:, at] = dot_nt(xs[p], wg[at, :])
                us[:, at] = dot_nt(xs[p], wu[at, :])
                return carry

            lax.fori_loop(0, wide // tile, one, 0)
            together = dot_nt(xs[p], ws[...])
            gs[:, wide:total] = together[:, :shared]
            us[:, wide:total] = together[:, shared:]

        def middle(p, k):
            step = 32

            def some(i, carry):
                at = pl.ds(pl.multiple_of(i * step, step), step)
                lane = lax.broadcasted_iota(jnp.int32, (step, 128), 1)
                expert = lax.rem(lane, 64)
                mixed = mixs[p, at].astype(jnp.float32)
                first = jnp.sum(jnp.where(expert == 2 * e, mixed, 0.0), axis=1, keepdims=True)
                second = jnp.sum(jnp.where(expert == 2 * e + 1, mixed, 0.0), axis=1, keepdims=True)

                def part(lo, hi, weight, to_gate, to_up):
                    gate, up = gs[at, lo:hi], us[at, lo:hi]
                    grad = dh[p, at, lo:hi].astype(jnp.float32)
                    logistic = sigmoid(gate)
                    active = gate * logistic
                    value = active * up
                    share = jnp.sum(value * grad, axis=1, keepdims=True)
                    grad = grad * weight
                    dh[p, at, lo:hi] = (value * weight).astype(low)
                    dgu[at, to_gate : to_gate + hi - lo] = (grad * up * (logistic + active * (1.0 - logistic))).astype(low)
                    dgu[at, to_up : to_up + hi - lo] = (grad * active).astype(low)
                    return share

                one = part(0, segment, first, 0, wide)
                two = part(segment, wide, second, segment, wide + segment)
                part(wide, total, 1.0, 2 * wide, 2 * wide + shared)
                shares = jnp.where(lane == 2 * e, one, jnp.where(lane == 2 * e + 1, two, 0.0))
                grads[k, at, width:full] = shares.astype(low)
                return carry

            lax.fori_loop(0, pair // step, some, 0)

        def inputs(p, k, first, count):
            def one(n, carry):
                at = at_tile(n, first)
                value = matmul(dgu[:, :wide], wg[:, at]) + matmul(dgu[:, wide : 2 * wide], wu[:, at])
                grads[k, :, at] = (value + matmul(dgu[:, 2 * wide :], ws[:, at])).astype(low)
                return carry

            lax.fori_loop(0, count // tile, one, 0)

        def outputs(p, k):
            if k > 1:
                keep_out[k - 2].wait()

            def one(n, carry):
                at = at_tile(n)
                value = matmul(dh[p, :, :wide], wd[:, at]) + matmul(dh[p, :, wide:], wc[:, at])
                ost[k % 2, :, at] = value.astype(low)
                return carry

            lax.fori_loop(0, width // tile, one, 0)
            keep_out[k].start()

        def compute(k):
            p = pairs[k]
            keep[k].start()
            hidden(p, k)
            if k > 0:
                keep_dgu[k - 1].wait()
            middle(p, k)
            keep_dgu[k].start()
            keep_hm[k].start()
            inputs(p, k, 0, half)
            give[k][0].start()
            inputs(p, k, half, half)
            give[k][1].start()

        def chip(k, part):
            give[k][part].wait_recv()
            cut = cuts[part]
            add_block(grads.at[k, mine, cut], grads.at[k, mine, cut], theirs.at[k, :, cut], length)

        for load in load_out:
            load.wait()
        for k in range(4):
            load_dy[k].wait()
            back(pairs[k])
        for load in load_in:
            load.wait()
        for move in moves:
            move["load"].wait()
            move["p"].wait_recv()
        compute(0)
        for move in moves:
            move["x"].wait_recv()
            move["lo"].start()
            move["px"].start()
        for move in moves:
            move["y"].wait_recv()
            move["hi"].start()
            move["py"].start()
        chip(0, 0)
        chip(0, 1)
        for move in moves:
            move["px"].wait_recv()
        compute(1)
        for move in moves:
            move["lo"].wait_recv()
            move["plo"].start()
            move["hi"].wait_recv()
            move["phi"].start()
        chip(1, 0)
        a1.start()
        chip(1, 1)
        for move in moves:
            move["py"].wait_recv()
        compute(2)
        chip(2, 1)
        b1.start()
        chip(2, 0)
        for move in moves:
            move["plo"].wait_recv()
            move["phi"].wait_recv()
        compute(3)
        chip(3, 0)
        a0.start()
        chip(3, 1)
        b0.start()
        outputs(pairs[0], 0)
        outputs(pairs[1], 1)
        outputs(pairs[2], 2)
        a0.wait_recv()
        add_block(turn.at[:, a], grads.at[2, mine, a], near.at[1, :, a], length)
        ta.start()
        b0.wait_recv()
        add_block(turn.at[:, b], grads.at[1, mine, b], near.at[1, :, b], length)
        tb.start()
        outputs(pairs[3], 3)
        a1.wait_recv()
        b1.wait_recv()
        ta.wait_recv()
        tb.wait_recv()

        def sum_up(i, carry):
            at = pl.ds(pl.multiple_of(i * 16, 16), 16)
            here = pl.ds(pl.multiple_of(core * length + i * 16, 16), 16)
            value = grads[0, here].astype(jnp.float32) + near[0, at].astype(jnp.float32)
            value = (value + last[at].astype(jnp.float32)).astype(low)
            own[at] = value[:, :width]
            own_mix[at] = value[:, width:]
            return carry

        lax.fori_loop(0, length // 16, sum_up, 0)
        for move in moves:
            for name in ("x", "y", "p", "lo", "hi", "px", "py", "plo", "phi"):
                move[name].wait_send()
        for k in range(4):
            for each in give[k]:
                each.wait_send()
            keep[k].wait()
            keep_hm[k].wait()
        keep_dgu[3].wait()
        keep_out[2].wait()
        keep_out[3].wait()
        for each in (a0, a1, b0, b1, ta, tb):
            each.wait_send()

    shape = jax.ShapeDtypeStruct
    vmem = pltpu.VMEM
    return pl.pallas_call(
        kernel,
        out_shape=[
            shape((4, pair, width), low),
            shape((4, pair, width), low),
            shape((4, pair, total), low),
            shape((4, pair, both), low),
            shape((length, width), low),
            shape((length, 128), low),
        ],
        in_specs=[ANY] * 9,
        out_specs=[ANY] * 4 + [VMEM] * 2,
        scratch_shapes=[
            vmem((4, pair, width), low),
            vmem((4, pair, 128), low),
            vmem((4, pair, width), low),
            vmem((wide, width), low),
            vmem((wide, width), low),
            vmem((2 * shared, width), low),
            vmem((wide, width), low),
            vmem((shared, width), low),
            vmem((4, pair, total), low),
            vmem((pair, both), low),
            vmem((pair, total), jnp.float32),
            vmem((pair, total), jnp.float32),
            vmem((2, pair, width), low),
            vmem((4, pair, full), low),
            vmem((4, length, full), low),
            vmem((2, length, full), low),
            vmem((length, full), low),
            vmem((length, full), low),
            pltpu.SemaphoreType.DMA((32,)),
            pltpu.SemaphoreType.DMA((32,)),
            pltpu.SemaphoreType.DMA((56,)),
        ],
        compiler_params=pltpu.CompilerParams(
            collective_id=cid, has_side_effects=True, vmem_limit_bytes=63 * 1024 * 1024
        ),
        name="expert_stage",
    )(rows, mixing, upstream.reshape(4, pair, width), gate, up, down, common_gate, common_up, common_down)


class Weights:
    sends, locals, load = 0, 80, 0.0

    def __init__(self, rows, grads, hidden, upstream, experts, units, common, own, at=0.0, pace=2.6):
        self.arrays = [rows, grads, hidden, upstream]
        self.in_spec = self.out_spec = ANY
        self.at, self.pace = at, pace
        self.tokens, self.width = rows.shape
        self.total = hidden.shape[1]
        self.experts, self.units, self.common, self.own = experts, units, common, own
        self.pad = lanes(units)
        self.wide = experts * self.pad
        self.shared = self.total - self.wide
        low = rows.dtype
        shape = jax.ShapeDtypeStruct
        whole, part = shape((experts, units, self.width), low), shape((self.width // own, common, own), low)
        self.outs = [whole, whole, whole, part, part, part]
        tile = pltpu.VMEM((2, experts, units, own), low)
        piece = pltpu.VMEM((2, common, own), low)
        self.scratch = [
            pltpu.VMEM(rows.shape, low),
            pltpu.VMEM(upstream.shape, low),
            pltpu.VMEM(hidden.shape, low),
            pltpu.VMEM(hidden.shape, low),
            pltpu.VMEM((self.total, self.tokens), low),
            pltpu.VMEM((2 * self.total, self.tokens), low),
            tile,
            tile,
            tile,
            piece,
            piece,
            piece,
        ]

    def plain(self):
        rows, grads, hidden, upstream = self.arrays
        low, wide, shared = rows.dtype, self.wide, self.shared
        into, out = matmul_tn(grads, rows).astype(low), matmul_tn(hidden, upstream).astype(low)

        def pick(array, first):
            return jnp.stack([array[first + i * self.pad :][: self.units] for i in range(self.experts)])

        def blocks(array, first):
            return array[first : first + self.common].reshape(self.common, -1, self.own).transpose(1, 0, 2)

        return [
            pick(into, 0),
            pick(into, wide),
            pick(out, 0),
            blocks(into, 2 * wide),
            blocks(into, 2 * wide + shared),
            blocks(out, wide),
        ]

    def steps(
        self, fab, x_h, g_h, h_h, y_h, gate_o, up_o, down_o, cg_o, cu_o, cd_o,
        xs, ys, s0, s1, ht, gt, gst, ust, dst, cgs, cus, cds,
    ):
        units, pad, wide, total, own, common = self.units, self.pad, self.wide, self.total, self.own, self.common
        columns = self.width // own
        load_h, load_y, load_x = fab.here(h_h, s0), fab.here(y_h, ys), fab.here(x_h, xs)
        load_lo = fab.here(g_h.at[:, pl.ds(0, total)], s1)
        load_hi = fab.here(g_h.at[:, pl.ds(total, total)], s0)

        def puts(n, whole, part):
            cols = pl.ds(n * own, own)
            copies = [fab.here(s.at[n % 2, i], o.at[i, :, cols]) for s, o in whole for i in range(self.experts)]
            return copies + [fab.here(s.at[n % 2], o.at[n]) for s, o in part]

        put_in = [puts(n, ((gst, gate_o), (ust, up_o)), ((cgs, cg_o), (cus, cu_o))) for n in range(columns)]
        put_out = [puts(n, ((dst, down_o),), ((cds, cd_o),)) for n in range(columns)]

        def begin():
            for each in (load_h, load_y, load_lo, load_x):
                each.start()

        def turn(dst_ref, src_ref, first):
            for at in range(0, total, 128):
                dst_ref[first + at : first + at + 128, :] = src_ref[:, at : at + 128].T

        def turn_hidden():
            load_h.wait()
            turn(ht, s0, 0)
            load_hi.start()

        def turn_lo():
            load_lo.wait()
            turn(gt, s1, 0)

        def turn_hi():
            load_hi.wait()
            turn(gt, s0, total)

        def store(stage, n, value):
            for i in range(self.experts):
                stage[n % 2, i] = value[i * pad : i * pad + units].astype(stage.dtype)

        def down(n):
            def step():
                if n == 0:
                    load_y.wait()
                if n >= 2:
                    for each in put_out[n - 2]:
                        each.wait()
                value = matmul(ht[...], ys[:, n * own : (n + 1) * own])
                store(dst, n, value)
                cds[n % 2] = value[wide : wide + common].astype(cds.dtype)
                for each in put_out[n]:
                    each.start()

            return step

        def gate(n):
            def step():
                if n == 0:
                    load_x.wait()
                if n >= 2:
                    for each in put_in[n - 2]:
                        each.wait()
                store(gst, n, matmul(gt[:wide], xs[:, n * own : (n + 1) * own]))

            return step

        def up(n):
            def step():
                value = matmul(gt[wide:], xs[:, n * own : (n + 1) * own])
                store(ust, n, value)
                cgs[n % 2] = value[wide : wide + common].astype(cgs.dtype)
                cus[n % 2] = value[wide + self.shared : wide + self.shared + common].astype(cus.dtype)
                for each in put_in[n]:
                    each.start()

            return step

        def end():
            for each in (*put_out[-2], *put_out[-1], *put_in[-2], *put_in[-1]):
                each.wait()

        t, p = self.at, self.pace
        result = [(t, begin), (t + 3, turn_hidden)]
        t += 4
        for n in range(columns):
            result.append((t, down(n)))
            t += 0.7 * p
        result.append((t, turn_lo))
        t += 0.7 * p
        result.append((t, turn_hi))
        t += 0.7 * p
        for n in range(columns):
            result.append((t, gate(n)))
            t += 0.6 * p
            result.append((t, up(n)))
            t += 0.8 * p
        result.append((1e9, end))
        return result


class Attend:
    names = ("sum", "normed", "query_nope", "query_rope", "latent_raw", "compressed", "key_rope", "expanded", "weights", "attended")

    def __init__(self, hidden, pre_gain, latent_gain, cosine, sine, segments, query, latent, expand, output, at=0.0):
        length = hidden.shape[0]
        self.heads = query.shape[1] // (HEAD_DIM + ROPE_DIM)
        self.at = at
        low = hidden.dtype
        shape = jax.ShapeDtypeStruct
        self.arrays = [
            hidden, pre_gain[None], latent_gain[None], cosine, sine, segments[:, None], segments[None],
            query, latent, expand, output,
        ]
        self.in_specs = [VMEM] * 7 + [ANY] * 4
        self.out_spec = VMEM
        heads = self.heads
        self.line = Line(shape(hidden.shape, low), at=at)
        self.outs = [
            shape(hidden.shape, low),
            shape(hidden.shape, low),
            shape((length, heads * HEAD_DIM), low),
            shape((length, heads * ROPE_DIM), low),
            shape((length, KV_RANK), jnp.float32),
            shape((length, KV_RANK), low),
            shape((length, ROPE_DIM), low),
            shape((length, heads * 2 * HEAD_DIM), low),
            shape((heads, length, length), jnp.float32),
            shape((length, heads * HEAD_DIM), low),
        ]
        self.scratch = [pltpu.VMEM(w.shape, low) for w in (query, latent, expand, output)]
        self.scratch += [pltpu.VMEM((length, query.shape[1]), jnp.float32), pltpu.VMEM(hidden.shape, low)] + self.line.scratch
        self.sends, self.locals, self.load = self.line.sends, 4, self.line.load

    def steps(
        self, fab, x, pre_gain, latent_gain, cos, sin, seg_col, seg_row, q_h, l_h, e_h, o_h,
        out, normed, q_nope, q_rope, raw, compressed, k_rope, expanded, probs, attended,
        wq, wl, we, wo, qs, part, mixed, from_end, from_mid,
    ):
        length = x.shape[0]
        loads = [fab.here(a, b) for a, b in ((l_h, wl), (q_h, wq), (e_h, we), (o_h, wo))]
        low = jnp.bfloat16
        scale = 1.0 / math.sqrt(HEAD_DIM + ROPE_DIM)

        def begin():
            for each in loads:
                each.start()

        def norm():
            def some(i, carry):
                at = pl.ds(pl.multiple_of(i * 32, 32), 32)
                v = x[at].astype(jnp.float32)
                inverse = lax.rsqrt(jnp.mean(v * v, axis=1, keepdims=True) + EPSILON)
                normed[at] = (v * inverse * pre_gain[...]).astype(low)
                return carry

            lax.fori_loop(0, length // 32, some, 0)

        def latent():
            loads[0].wait()
            every = dot_nt(normed[...], wl[...])
            value = every[:, :KV_RANK]
            raw[...] = value
            inverse = lax.rsqrt(jnp.mean(value * value, axis=1, keepdims=True) + EPSILON)
            compressed[...] = (value * inverse * latent_gain[...]).astype(low)
            k_rope[...] = rotate(every[:, KV_RANK:], cos[...], sin[...]).astype(low)

        def queries():
            loads[1].wait()

            def one(n, carry):
                at = pl.ds(pl.multiple_of(n * 256, 256), 256)
                qs[:, at] = matmul(normed[...], wq[:, at])
                return carry

            lax.fori_loop(0, qs.shape[1] // 256, one, 0)
            for h in range(self.heads):
                first = h * (HEAD_DIM + ROPE_DIM)
                q_nope[:, h * HEAD_DIM : (h + 1) * HEAD_DIM] = qs[:, first : first + HEAD_DIM].astype(low)
                turned = rotate(qs[:, first + HEAD_DIM : first + HEAD_DIM + ROPE_DIM], cos[...], sin[...])
                q_rope[:, h * ROPE_DIM : (h + 1) * ROPE_DIM] = turned.astype(low)

        def expand():
            loads[2].wait()
            for n in range(0, expanded.shape[1], 256):
                expanded[:, n : n + 256] = matmul(compressed[...], we[:, n : n + 256]).astype(low)

        def head(h):
            def step():
                first = 2 * HEAD_DIM * h
                scores = dot_nt(q_nope[:, h * HEAD_DIM : (h + 1) * HEAD_DIM], expanded[:, first : first + HEAD_DIM])
                scores = scores + dot_nt(q_rope[:, h * ROPE_DIM : (h + 1) * ROPE_DIM], k_rope[...])
                row = lax.broadcasted_iota(jnp.int32, (length, length), 0)
                column = lax.broadcasted_iota(jnp.int32, (length, length), 1)
                allowed = jnp.logical_and(column <= row, seg_col[...] == seg_row[...])
                scores = jnp.where(allowed, scores * scale, MASKED)
                raised = jnp.exp(scores - jnp.max(scores, axis=1, keepdims=True))
                chance = raised / jnp.sum(raised, axis=1, keepdims=True)
                probs[h] = chance
                value = matmul(chance.astype(low), expanded[:, first + HEAD_DIM : first + 2 * HEAD_DIM])
                attended[:, h * HEAD_DIM : (h + 1) * HEAD_DIM] = value.astype(low)

            return step

        def project():
            loads[3].wait()

            def one(n, carry):
                at = pl.ds(pl.multiple_of(n * 256, 256), 256)
                part[:, at] = matmul(attended[...], wo[:, at]).astype(low)
                return carry

            lax.fori_loop(0, part.shape[1] // 256, one, 0)

        t = self.at
        result = [(t, begin), (t + 0.1, norm), (t + 1, latent), (t + 3, queries), (t + 6, expand)]
        result += [(t + 7 + h, head(h)) for h in range(self.heads)]
        result.append((t + 12, project))
        self.line.at, self.line.wait = t + 14, 0.0
        return result + self.line.steps(fab, part, out, mixed, from_end, from_mid)


class Tail:
    sends, load = 0, 0.0

    def __init__(self, latent_line, normed_line, raw, latent_gain, normed, latent, hidden, pre_gain, grad_middle, small, at=0.0):
        self.at = at
        self.latent_line, self.normed_line = latent_line, normed_line
        self.arrays = [raw, latent_gain[None], normed, latent, hidden, pre_gain[None], grad_middle, small]
        self.in_spec = self.out_spec = VMEM
        low = hidden.dtype
        length, width = hidden.shape
        self.outs = [jax.ShapeDtypeStruct(hidden.shape, low)]
        depth = lanes(latent.shape[0])
        self.scratch = [
            pltpu.VMEM((length, depth), low),
            pltpu.VMEM((depth, length), low),
            pltpu.VMEM((latent.shape[0], width), low),
            pltpu.VMEM(small.shape, jnp.float32),
            pltpu.VMEM((length, width), jnp.float32),
            pltpu.VMEM((1, width), jnp.float32),
        ]
        self.locals = 1

    def latent_source(self):
        return self.refs[11]

    def small_source(self):
        return self.refs[12]

    def steps(self, fab, raw, latent_gain, normed, latent, hidden, pre_gain, grad_middle, small, out, gl, turned, lg, sm, gn, pre):
        latent_sum, normed_sum = self.latent_line.refs[1], self.normed_line.refs[1]
        length, width = hidden.shape
        rank = raw.shape[1]
        low = gl.dtype
        tile = 256

        def latent_back():
            grad, value = latent_sum[:, :rank].astype(jnp.float32), raw[...]
            inverse = lax.rsqrt(jnp.mean(value * value, axis=1, keepdims=True) + EPSILON)
            gain_part = jnp.sum(grad * value * inverse, axis=0, keepdims=True)
            scaled = grad * latent_gain[...]
            inner = jnp.mean(scaled * value, axis=1, keepdims=True)
            gl[:, :rank] = (inverse * scaled - value * (inverse * inverse * inverse * inner)).astype(low)
            gl[:, rank:] = latent_sum[:, rank:]
            sm[...] = small[...]
            part = rank // 8
            for j in range(8):
                sm[j, 2:3, :part] = gain_part[:, j * part : (j + 1) * part]
            for n in range(0, gl.shape[1], 128):
                turned[n : n + 128, :] = gl[:, n : n + 128].T
            pre[...] = jnp.zeros_like(pre)

        def latent_grad(quarter):
            def one(n, carry):
                at = pl.ds(pl.multiple_of(n * tile, tile), tile)
                lg[:, at] = matmul(turned[: lg.shape[0], :], normed[:, at]).astype(low)
                return carry

            count = width // tile // 4
            return lambda: lax.fori_loop(quarter * count, (quarter + 1) * count, one, 0)

        def normed_grad(quarter):
            def one(n, carry):
                at = pl.ds(pl.multiple_of(n * tile, tile), tile)
                gn[:, at] = normed_sum[:, at].astype(jnp.float32) + matmul(gl[:, : latent.shape[0]], latent[:, at])
                return carry

            count = width // tile // 4
            return lambda: lax.fori_loop(quarter * count, (quarter + 1) * count, one, 0)

        def normed_back(quarter):
            def some(i, carry):
                at = pl.ds(pl.multiple_of(i * 16, 16), 16)
                value, grad = hidden[at].astype(jnp.float32), gn[at]
                inverse = lax.rsqrt(jnp.mean(value * value, axis=1, keepdims=True) + EPSILON)
                pre[...] += jnp.sum(grad * value * inverse, axis=0, keepdims=True)
                scaled = grad * pre_gain[...]
                inner = jnp.mean(scaled * value, axis=1, keepdims=True)
                back = inverse * scaled - value * (inverse * inverse * inverse * inner)
                out[at] = (grad_middle[at] + back).astype(low)
                return carry

            count = length // 16 // 4
            return lambda: lax.fori_loop(quarter * count, (quarter + 1) * count, some, 0)

        def gain_grad():
            part = width // 8
            for j in range(8):
                sm[j, 0:1, :] = pre[:, j * part : (j + 1) * part]

        t = self.latent_line.finish() + 0.1
        result = [(t, latent_back)] + [(t + 1.5 + 0.8 * i, latent_grad(i)) for i in range(4)]
        t = self.normed_line.finish() + 0.1
        result += [(t + 0.8 * i, normed_grad(i)) for i in range(4)]
        result += [(t + 3.2 + 1.2 * i, normed_back(i)) for i in range(4)]
        result.append((t + 8.0, gain_grad))
        return result


def lanes(width):
    return -(-width // 128) * 128


def pad_to(array, axis, size):
    widths = [(0, 0)] * array.ndim
    widths[axis] = (0, size - array.shape[axis])
    return jnp.pad(array, widths) if widths[axis][1] else array


def shards(
    hidden_in,
    segment_ids,
    expert_ids,
    query_weight,
    latent_weight,
    expand_weight,
    output_weight,
    prenorm,
    latentnorm,
    postnorm,
    router_weight,
    shared_gate,
    shared_up,
    shared_down,
    expert_gate,
    expert_up,
    expert_down,
    cotangent,
):
    groups = lax.axis_size("expert")
    ranks = lax.axis_size("tensor")
    fast = groups == 8 and ranks == 4
    me = lax.axis_index("expert")
    local_experts, _, units = expert_gate.shape
    experts = local_experts * groups
    length = hidden_in.shape[0]
    tokens = groups * length
    own_d = prenorm.shape[0]
    own_latent = latentnorm.shape[0]
    common = shared_gate.shape[1] // groups
    unit_pad, common_pad = lanes(units), lanes(common)
    low = jnp.bfloat16

    small = jnp.concatenate(
        [
            prenorm[None],
            postnorm[None],
            pad_to(latentnorm[None], 1, own_d),
            jnp.zeros((5, own_d), low),
            router_weight.T,
        ],
        axis=0,
    )
    small_full, latent_full, query_full, expand_full, output_full = exchange(
        [
            Gather(small, at=0.0),
            Gather(latent_weight.T, axis=1, at=0.1),
            Gather(query_weight, at=0.2),
            Gather(expand_weight, at=0.3),
            Gather(output_weight, axis=1, at=0.4),
        ],
        0,
        fast,
    )
    query_full = query_full.reshape(D, -1)
    expand_full = expand_full.reshape(KV_RANK, -1)
    pre_gain = small_full[:, 0].reshape(D).astype(jnp.float32)
    post_gain = small_full[:, 1].reshape(D).astype(jnp.float32)
    latent_gain = small_full[:, 2, :own_latent].reshape(KV_RANK).astype(jnp.float32)
    router_full = small_full[:, 8:].transpose(1, 0, 2).reshape(experts, D)

    heads = query_full.shape[1] // (HEAD_DIM + ROPE_DIM)
    hidden = hidden_in.astype(jnp.float32)
    cosine, sine = rotary_tables(length)
    inverse_pre = lax.rsqrt(jnp.mean(hidden * hidden, axis=1, keepdims=True) + EPSILON)
    scale = 1.0 / math.sqrt(HEAD_DIM + ROPE_DIM)
    segments = segment_ids[0]

    def unit_blocks(weight):
        return weight.reshape(groups, common, own_d)

    beside = [
        Gather(cotangent, at=0.1),
        Swap(unit_blocks(shared_gate.T), at=0.2),
        Swap(unit_blocks(shared_up.T), at=0.3),
        Swap(unit_blocks(shared_down), at=0.4),
    ]
    if fast:
        attend = Attend(
            hidden_in, pre_gain, latent_gain, cosine, sine, segments, query_full, latent_full, expand_full, output_full,
            at=0.5,
        )
        (
            upstream_all,
            common_gate,
            common_up,
            common_down,
            attention,
            normed,
            query_nope,
            query_rope,
            latent_raw,
            compressed,
            key_rope,
            expanded,
            probabilities,
            attended,
        ) = exchange([*beside, attend], 1, fast)
    else:
        normed = (hidden * inverse_pre * pre_gain).astype(low)
        query_raw = matmul(normed, query_full).reshape(length, heads, HEAD_DIM + ROPE_DIM)
        query_nope = query_raw[:, :, :HEAD_DIM].astype(low)
        query_rope = rotate(query_raw[:, :, HEAD_DIM:], cosine[:, None, :], sine[:, None, :]).astype(low)
        latent_all = matmul_nt(normed, latent_full)
        latent_raw = latent_all[:, :KV_RANK]
        norm_latent = lax.rsqrt(jnp.mean(latent_raw * latent_raw, axis=1, keepdims=True) + EPSILON)
        compressed = (latent_raw * norm_latent * latent_gain).astype(low)
        key_rope = rotate(latent_all[:, KV_RANK:], cosine, sine).astype(low)
        expanded = matmul(compressed, expand_full).astype(low)
        parts = expanded.reshape(length, heads, 2 * HEAD_DIM)
        position = jnp.arange(length)
        allowed = (position[None, :] <= position[:, None]) & (segments[:, None] == segments[None, :])
        raw = jnp.einsum("qhd,khd->hqk", query_nope, parts[:, :, :HEAD_DIM], preferred_element_type=jnp.float32)
        raw = raw + jnp.einsum("qhr,kr->hqk", query_rope, key_rope, preferred_element_type=jnp.float32)
        scores = jnp.where(allowed[None], raw * scale, MASKED)
        raised = jnp.exp(scores - jnp.max(scores, axis=2, keepdims=True))
        probabilities = raised / jnp.sum(raised, axis=2, keepdims=True)
        attended = (
            jnp.einsum(
                "hqk,khd->qhd", probabilities.astype(low), parts[:, :, HEAD_DIM:], preferred_element_type=jnp.float32
            )
            .astype(low)
            .reshape(length, heads * HEAD_DIM)
        )
        upstream_all, common_gate, common_up, common_down, attention = exchange(
            [*beside, Line(matmul(attended, output_full).astype(low))], 1, fast
        )
    query_nope = query_nope.reshape(length, heads, HEAD_DIM)
    query_rope = query_rope.reshape(length, heads, ROPE_DIM)
    key_nope = expanded.reshape(length, heads, 2 * HEAD_DIM)[:, :, :HEAD_DIM]
    values = expanded.reshape(length, heads, 2 * HEAD_DIM)[:, :, HEAD_DIM:]
    probabilities_low = probabilities.astype(low)
    inverse_latent = lax.rsqrt(jnp.mean(latent_raw * latent_raw, axis=1, keepdims=True) + EPSILON)
    middle = hidden + attention.astype(jnp.float32)
    inverse_post = lax.rsqrt(jnp.mean(middle * middle, axis=1, keepdims=True) + EPSILON)
    normed_mid = (middle * inverse_post * post_gain).astype(low)
    affinity = sigmoid(matmul_nt(normed_mid, router_full))
    chosen = jnp.any(
        expert_ids[:, :, None] == jnp.arange(experts, dtype=jnp.int32)[None, None, :], axis=1
    ).astype(jnp.float32)
    selected = chosen * affinity
    selected_total = jnp.sum(selected, axis=1, keepdims=True)
    mixing = ROUTE_SCALE * selected / selected_total

    upstream_rows = upstream_all.reshape(tokens, D)
    gate_rows, up_rows = expert_gate.transpose(0, 2, 1), expert_up.transpose(0, 2, 1)
    wide = local_experts * unit_pad
    total = wide + common_pad
    if fast:
        high = mixing.astype(low)
        rest = (mixing - high.astype(jnp.float32)).astype(low)
        pair = jnp.concatenate([pad_to(high, 1, 64), pad_to(rest, 1, 64)], axis=1)
        mixture_rows, token_rows, mixed_hidden, grad_both, grad_own, mixing_grad_own = expert_stage(
            normed_mid,
            pair,
            upstream_all,
            gate_rows,
            up_rows,
            expert_down,
            common_gate,
            common_up,
            common_down,
            2,
        )
        token_rows = token_rows.reshape(tokens, D)
        mixed_hidden = mixed_hidden.reshape(tokens, total)
        grad_both = grad_both.reshape(tokens, 2 * total)
    else:
        token_rows = lax.all_gather(normed_mid, "expert", axis=0, tiled=True)
        mixing_own = lax.dynamic_slice_in_dim(
            lax.all_gather(mixing, "expert", axis=0, tiled=True), me * local_experts, local_experts, axis=1
        )
        segment = jnp.minimum(jnp.arange(total) // unit_pad, local_experts)
        scales = jnp.concatenate([mixing_own, jnp.ones((tokens, 1), jnp.float32)], axis=1)
        mixing_wide = sum(
            jnp.where(segment[None, :] == i, scales[:, i : i + 1], 0.0) for i in range(local_experts + 1)
        )

        def padded(weight):
            return jnp.concatenate([pad_to(weight[i], 0, unit_pad) for i in range(local_experts)], axis=0)

        def joined(blocks):
            return pad_to(blocks.transpose(1, 0, 2).reshape(common, D), 0, common_pad)

        weight_in = jnp.concatenate([padded(gate_rows), padded(up_rows), joined(common_gate), joined(common_up)], axis=0)
        weight_out = jnp.concatenate([padded(expert_down), joined(common_down)], axis=0)
        every = matmul_nt(token_rows, weight_in)
        gate = jnp.concatenate([every[:, :wide], every[:, 2 * wide : 2 * wide + common_pad]], axis=1)
        up = jnp.concatenate([every[:, wide : 2 * wide], every[:, 2 * wide + common_pad :]], axis=1)
        logistic = sigmoid(gate)
        unit_hidden = gate * logistic * up
        mixed_hidden = (unit_hidden * mixing_wide).astype(low)
        mixture_rows = matmul(mixed_hidden, weight_out).astype(low)
        grad_unit = matmul_nt(upstream_rows, weight_out)
        mixing_share = unit_hidden * grad_unit
        mixing_grad = jnp.stack(
            [jnp.sum(mixing_share[:, i * unit_pad : (i + 1) * unit_pad], axis=1) for i in range(local_experts)], axis=1
        )
        grad_hidden = grad_unit * mixing_wide
        grad_up = (grad_hidden * gate * logistic).astype(low)
        grad_gate = (grad_hidden * up * logistic * (1.0 + gate * (1.0 - logistic))).astype(low)
        grad_both = jnp.concatenate(
            [grad_gate[:, :wide], grad_up[:, :wide], grad_gate[:, wide:], grad_up[:, wide:]], axis=1
        )
        spread = jnp.arange(lanes(experts))
        mixing_grad_wide = sum(
            jnp.where(spread[None, :] == me * local_experts + i, mixing_grad[:, i : i + 1], 0.0)
            for i in range(local_experts)
        ).astype(low)
        grad_own = lax.psum_scatter(matmul(grad_both, weight_in).astype(low), "expert", tiled=True)
        mixing_grad_own = lax.psum_scatter(mixing_grad_wide, "expert", tiled=True)
    (
        grad_mid,
        grad_mixing,
        mixture_own,
        expert_gate_grad,
        expert_up_grad,
        expert_down_grad,
        common_gate_grad,
        common_up_grad,
        common_down_grad,
    ) = exchange(
        [
            Line(grad_own),
            Line(mixing_grad_own, pieces=1, at=-0.1),
            Scatter(mixture_rows.reshape(groups, length, D), pieces=4, at=0.2),
            Weights(
                token_rows, grad_both, mixed_hidden, upstream_rows, local_experts, units, common, own_d, at=1.0
            ),
        ],
        4,
        fast,
    )
    grad_mid = grad_mid.astype(jnp.float32)
    grad_mixing = grad_mixing[:, :experts].astype(jnp.float32)
    grad_selected = (
        ROUTE_SCALE
        * chosen
        * (
            grad_mixing / selected_total
            - jnp.sum(grad_mixing * selected, axis=1, keepdims=True) / (selected_total * selected_total)
        )
    )
    grad_logits = (grad_selected * affinity * (1.0 - affinity)).astype(low)
    router_grad = matmul_tn(grad_logits, normed_mid)
    grad_mid = grad_mid + matmul(grad_logits, router_full)
    upstream = cotangent.astype(jnp.float32)
    grad_middle_norm, post_grad = norm_backward(grad_mid, middle, inverse_post, post_gain)
    grad_middle = upstream + grad_middle_norm
    grad_attention = grad_middle.astype(low)
    output_grad = matmul_tn(attended, grad_attention)
    grad_attended = matmul_nt(grad_attention, output_full).astype(low).reshape(length, heads, HEAD_DIM)
    grad_probs = jnp.einsum("qhd,khd->hqk", grad_attended, values, preferred_element_type=jnp.float32)
    inner = jnp.sum(probabilities * grad_probs, axis=2, keepdims=True)
    grad_scores = (probabilities * (grad_probs - inner)).astype(low)
    grad_query_nope = scale * jnp.einsum("hqk,khd->qhd", grad_scores, key_nope, preferred_element_type=jnp.float32)
    grad_query_rope = scale * jnp.einsum("hqk,kr->qhr", grad_scores, key_rope, preferred_element_type=jnp.float32)
    grad_key_nope = scale * jnp.einsum("hqk,qhd->khd", grad_scores, query_nope, preferred_element_type=jnp.float32)
    grad_key_rope = scale * jnp.einsum("hqk,qhr->kr", grad_scores, query_rope, preferred_element_type=jnp.float32)
    grad_values = jnp.einsum("hqk,qhd->khd", probabilities_low, grad_attended, preferred_element_type=jnp.float32)
    grad_query = (
        jnp.concatenate(
            [grad_query_nope, rotate(grad_query_rope, cosine[:, None, :], -sine[:, None, :])], axis=2
        )
        .astype(low)
        .reshape(length, heads * (HEAD_DIM + ROPE_DIM))
    )
    query_grad = matmul_tn(normed, grad_query)
    grad_expanded = (
        jnp.concatenate([grad_key_nope, grad_values], axis=2).astype(low).reshape(length, heads * 2 * HEAD_DIM)
    )
    expand_grad = matmul_tn(compressed, grad_expanded)
    grad_key = pad_to(rotate(grad_key_rope, cosine, -sine), 1, lanes(ROPE_DIM))
    grad_latent_terms = jnp.concatenate([matmul_nt(grad_expanded, expand_full), grad_key], axis=1).astype(low)
    small_grad = jnp.concatenate(
        [
            jnp.zeros((groups, 1, own_d), jnp.float32),
            post_grad.reshape(groups, 1, own_d),
            jnp.zeros((groups, 14, own_d), jnp.float32),
            router_grad.reshape(experts, groups, own_d).transpose(1, 0, 2),
        ],
        axis=1,
    )
    latent_line = Line(grad_latent_terms, at=0.0, early=True)
    normed_line = Line(matmul_nt(grad_query, query_full).astype(low), at=0.05, early=True)
    dense = [
        Scatter(query_grad.astype(low).reshape(groups, own_d, -1), pieces=2, at=0.2),
        Scatter(expand_grad.astype(low).reshape(groups, own_latent, -1), at=0.4),
        Scatter(output_grad.astype(low), axis=1, pieces=2, at=0.6),
    ]
    swaps = [
        Swap(common_gate_grad, at=30.0),
        Swap(common_up_grad, at=30.1),
        Swap(common_down_grad, at=30.2),
    ]
    if fast:
        tail = Tail(
            latent_line, normed_line, latent_raw, latent_gain, normed, latent_full, hidden_in, pre_gain, grad_middle,
            small_grad,
        )
        shape = jax.ShapeDtypeStruct
        (
            _,
            _,
            query_out,
            expand_out,
            output_out,
            common_gate_out,
            common_up_out,
            common_down_out,
            mixture,
            latent_out,
            small_out,
            input_gradient,
        ) = exchange(
            [
                latent_line,
                normed_line,
                *dense,
                *swaps,
                Line(mixture_own, at=0.1),
                Scatter(shape((latent_full.shape[0], D), low), axis=1, pieces=2, at=24.0, source=tail.latent_source),
                Scatter(shape(small_grad.shape, jnp.float32), at=51.5, source=tail.small_source),
                tail,
            ],
            5,
            fast,
        )
    else:
        grad_latent_sum, grad_normed_sum, query_out, expand_out, output_out = exchange(
            [latent_line, normed_line, *dense], 5, fast
        )
        grad_latent_sum = grad_latent_sum.astype(jnp.float32)
        grad_latent_raw, latent_norm_grad = norm_backward(
            grad_latent_sum[:, :KV_RANK], latent_raw, inverse_latent, latent_gain
        )
        grad_latent = jnp.concatenate(
            [grad_latent_raw, grad_latent_sum[:, KV_RANK : KV_RANK + ROPE_DIM]], axis=1
        ).astype(low)
        latent_grad = matmul_tn(grad_latent, normed)
        grad_normed = grad_normed_sum.astype(jnp.float32) + matmul(grad_latent, latent_full)
        grad_hidden_in, pre_grad = norm_backward(grad_normed, hidden, inverse_pre, pre_gain)
        input_gradient = (grad_middle + grad_hidden_in).astype(low)
        small_grad = small_grad.at[:, 0].set(pre_grad.reshape(groups, own_d))
        small_grad = small_grad.at[:, 2, :own_latent].set(latent_norm_grad.reshape(groups, own_latent))
        mixture, latent_out, small_out, common_gate_out, common_up_out, common_down_out = exchange(
            [
                Line(mixture_own),
                Scatter(latent_grad.astype(low), axis=1, pieces=2, at=0.2),
                Scatter(small_grad, at=0.1),
                *swaps,
            ],
            6,
            fast,
        )
    block_output = (middle + mixture.astype(jnp.float32)).astype(low)

    def unit_rows(back):
        return back.reshape(groups * common, own_d).astype(jnp.float32)

    return (
        block_output,
        input_gradient,
        query_out.astype(jnp.float32),
        latent_out.T.astype(jnp.float32),
        expand_out.astype(jnp.float32),
        output_out.astype(jnp.float32),
        small_out[0],
        small_out[2, :own_latent],
        small_out[1],
        small_out[16:].T,
        unit_rows(common_gate_out).T,
        unit_rows(common_up_out).T,
        unit_rows(common_down_out),
        expert_gate_grad.astype(jnp.float32).transpose(0, 2, 1),
        expert_up_grad.astype(jnp.float32).transpose(0, 2, 1),
        expert_down_grad.astype(jnp.float32),
    )


def solution(mesh):
    placed = (
        P("expert", None),
        P("expert", None),
        P("expert", None),
        P("expert", "tensor"),
        P("expert", None),
        P("expert", "tensor"),
        P("tensor", "expert"),
        P("expert"),
        P("expert"),
        P("expert"),
        P("expert", None),
        P("expert", "tensor"),
        P("expert", "tensor"),
        P("tensor", "expert"),
        P("expert", None, "tensor"),
        P("expert", None, "tensor"),
        P("expert", "tensor", None),
        P("expert", None),
    )
    return jax.shard_map(
        shards,
        mesh=mesh,
        in_specs=placed,
        out_specs=(
            P("expert", None),
            P("expert", None),
            P("expert", "tensor"),
            P("expert", None),
            P("expert", "tensor"),
            P("tensor", "expert"),
            P("expert"),
            P("expert"),
            P("expert"),
            P("expert", None),
            P("expert", "tensor"),
            P("expert", "tensor"),
            P("tensor", "expert"),
            P("expert", None, "tensor"),
            P("expert", None, "tensor"),
            P("expert", "tensor", None),
        ),
        check_vma=False,
    )
```
